32 devices in a mesh: prob: 1 (over z), samp: 4 (over y), feat: 8 (over x, core).
Axes of the slice: x: 4, y: 4, z: 1, core: 2. Of those that a mesh axis runs over, the one named last changes fastest.
The devices are a block of a 4x4x8 slice.
Arguments:
- x_mat: bfloat16 [512, 1048576], P(('prob', 'samp'), 'feat')
- w_init: float32 [1048576, 32], P(('prob', 'feat'))
- targets: float32 [512, 32], P(('prob', 'samp'))
- step_size: float32 [1048576], P(('prob', 'feat'))
Outputs:
- output 1: float32 [1048576, 32], P(('prob', 'feat'))
- output 2: float32 [512, 32], P(('prob', 'samp'))
All inputs are finite; a program needn't handle non-finite values.
Results may differ from the reference program's by a relative error of at most 0.00281675.
Values are sent between devices in bfloat16 or wider.
A program may use at most 768 MiB of HBM per device.

```python
import math
import jax
import jax.numpy as jnp
from jax import lax

SAMPLES = 512
FEATURES = 1048576
TARGETS = 32
FEAT_BLOCKS = 8
SWEEPS = 4
COMBINE_WEIGHT = 0.8
RIDGE_SCALE = 0.1


def feature_steps(x_mat, spread, start_key):
    col_sq = jnp.sum(jnp.square(x_mat.astype(jnp.float32)), axis=0) / SAMPLES
    precond = spread / col_sq
    root_pre = jnp.sqrt(precond)
    start_dir = jax.random.normal(start_key, (FEATURES,), jnp.float32)
    start_dir = start_dir / jnp.sqrt(jnp.sum(start_dir * start_dir))

    def power_step(direction, unused):
        row_vals = jnp.dot(x_mat, (root_pre * direction).astype(jnp.bfloat16), preferred_element_type=jnp.float32)
        col_vals = root_pre * jnp.dot(row_vals.astype(jnp.bfloat16), x_mat, preferred_element_type=jnp.float32) / SAMPLES
        dir_norm = jnp.sqrt(jnp.sum(col_vals * col_vals))
        return col_vals / dir_norm, dir_norm

    final_dir, dir_norms = lax.scan(power_step, start_dir, None, length=30)
    return precond / dir_norms[-1]


def setup_inputs(seed: int = 0, part: int = 0) -> dict:
    part_key = jax.random.fold_in(jax.random.key(seed), part)
    key_list = jax.random.split(part_key, 8)
    factor_rank = 8
    shared_frac = 2.0 * factor_rank / SAMPLES
    factors = jax.random.normal(key_list[0], (SAMPLES, factor_rank), jnp.float32)
    loadings = jax.random.normal(key_list[1], (FEATURES, factor_rank), jnp.float32)
    noise_part = jax.random.normal(key_list[2], (SAMPLES, FEATURES), jnp.float32)
    shared = jnp.dot(factors, loadings.T)
    x_mat = (math.sqrt(shared_frac / factor_rank) * shared + math.sqrt(1.0 - shared_frac) * noise_part).astype(jnp.bfloat16)
    spread = jnp.exp2(jax.random.uniform(key_list[3], (FEATURES,), jnp.float32, -2.0, 2.0))
    step_size = feature_steps(x_mat, spread, key_list[4])
    z_mat = jax.random.normal(key_list[5], (SAMPLES, TARGETS), jnp.float32).astype(jnp.bfloat16)
    w_raw = lax.dot_general(x_mat, z_mat, (((0,), (0,)), ((), ())), preferred_element_type=jnp.float32)
    w_fit = jnp.dot(x_mat, w_raw.astype(jnp.bfloat16), preferred_element_type=jnp.float32)
    w_init = w_raw * (0.7 / jnp.sqrt(jnp.mean(w_fit * w_fit)))
    w_true = jax.random.normal(key_list[6], (FEATURES, TARGETS), jnp.float32).astype(jnp.bfloat16)
    y_signal = jnp.dot(x_mat, w_true, preferred_element_type=jnp.float32)
    y_noise = jax.random.normal(key_list[7], (SAMPLES, TARGETS), jnp.float32)
    targets = 0.8 * y_signal / jnp.sqrt(jnp.mean(y_signal * y_signal)) + 0.6 * y_noise
    return {"x_mat": x_mat, "w_init": w_init, "targets": targets, "step_size": step_size}


def block_sum(x_mat, weights):
    feat_len = FEATURES // FEAT_BLOCKS
    weights_low = weights.astype(jnp.bfloat16)

    def one_block(total, block):
        x_block = lax.dynamic_slice_in_dim(x_mat, block * feat_len, feat_len, axis=1)
        w_block = lax.dynamic_slice_in_dim(weights_low, block * feat_len, feat_len, axis=0)
        block_prod = jnp.dot(x_block, w_block, preferred_element_type=jnp.float32)
        return total + block_prod.astype(jnp.bfloat16).astype(jnp.float32), None

    total, unused = lax.scan(one_block, jnp.zeros((SAMPLES, TARGETS), jnp.float32), jnp.arange(FEAT_BLOCKS))
    return total


def reference(x_mat, w_init, targets, step_size):
    ridge = RIDGE_SCALE * FEATURES / SAMPLES
    start_resid = targets - block_sum(x_mat, w_init)

    def sweep(state, unused):
        weights, residual = state
        gradient = lax.dot_general(x_mat, residual.astype(jnp.bfloat16), (((0,), (0,)), ((), ())), preferred_element_type=jnp.float32) / SAMPLES
        delta = step_size[:, None] * (gradient - ridge * weights)
        weights = weights + COMBINE_WEIGHT * delta
        residual = residual - COMBINE_WEIGHT * block_sum(x_mat, delta)
        return (weights, residual), None

    (weights, residual), unused = lax.scan(sweep, (w_init, start_resid), None, length=SWEEPS)
    return weights, residual
```

```python
import functools

import jax
import jax.numpy as jnp
from jax import lax
from jax.experimental import pallas as pl
from jax.experimental.pallas import tpu as pltpu
from jax.sharding import PartitionSpec as P

SWEEPS = 4
COMBINE_WEIGHT = 0.8
RIDGE_SCALE = 0.1
CHUNKS = 16
SUB = 512
V_SLOTS = 4
MESH = pl.DeviceIdType.MESH
NT = (((1,), (1,)), ((), ()))


def kernel(ns, nf, x_hbm, wt_hbm, yt_ref, eta_hbm, wout, rout, xbuf, relay, wbuf, ebuf, vx, vw, usend, rsbuf, agbuf, rbuf, rstate,
           own_sem, w_sem, e_sem, v_sem, rel_s, rel_r, dir_s, dir_r, fwd_s, fwd_r, a_s, a_r, b_s, b_r, c_s, c_r,
           wl_sem, wd_s, wd_r, wf_s, wf_r):
    y, f = lax.axis_index("samp"), lax.axis_index("feat")
    rows, feat_len = x_hbm.shape
    targets = wt_hbm.shape[0]
    own = feat_len // ns
    chunk = own // CHUNKS
    half = CHUNKS // 2
    sub = min(SUB, chunk)
    samples = rows * ns
    inv = 1.0 / samples
    ridge = RIDGE_SCALE * (feat_len * nf) / samples
    up, down, far = lax.rem(y + 1, ns), lax.rem(y + ns - 1, ns), lax.rem(y + 2, ns)
    ring = (up, down)

    def cols(owner, k):
        return pl.ds(pl.multiple_of(owner * own + k * chunk, chunk), chunk)

    def rows_of(s):
        return pl.ds(pl.multiple_of(s * rows, rows), rows)

    def remote(src, dst, send, recv, axis, dev):
        return pltpu.make_async_remote_copy(src_ref=src, dst_ref=dst, send_sem=send, recv_sem=recv,
                                            device_id={axis: dev}, device_id_type=MESH)

    def own_copy(k):
        return pltpu.make_async_copy(x_hbm.at[:, cols(y, k)], xbuf.at[k, rows_of(y), :], own_sem.at[k])

    def w_load(k):
        return pltpu.make_async_copy(wt_hbm.at[:, cols(y, k)], wbuf.at[k], w_sem.at[k])

    def e_load(k):
        return pltpu.make_async_copy(eta_hbm.at[:, cols(y, k)], ebuf.at[k], e_sem.at[k])

    v_steps = ns * CHUNKS

    def v_cols(k):
        return pl.ds(pl.multiple_of(k * chunk, chunk), chunk)

    def v_load(k, slot):
        return (pltpu.make_async_copy(x_hbm.at[:, v_cols(k)], vx.at[slot], v_sem.at[0, slot]),
                pltpu.make_async_copy(wt_hbm.at[:, v_cols(k)], vw.at[slot], v_sem.at[1, slot]))

    def relay_copy(d, i):
        return remote(x_hbm.at[:, cols(far, 2 * i + d)], relay.at[d, i], rel_s.at[d, i], rel_r.at[d, i], "samp", ring[d])

    def direct_copy(d, k, place):
        return remote(x_hbm.at[:, cols(ring[d], k)], xbuf.at[k, rows_of(place), :], dir_s.at[d, k], dir_r.at[d, k], "samp", ring[d])

    def forward_copy(d, i, place):
        return remote(relay.at[d, i], xbuf.at[2 * i + d, rows_of(place), :], fwd_s.at[d, i], fwd_r.at[d, i], "samp", ring[d])

    def wd_copy(d, k, owner):
        return remote(wbuf.at[k], wout.at[:, cols(owner, k)], wd_s.at[d, k], wd_r.at[d, k], "samp", ring[d])

    def wf_copy(d, i, owner):
        part = wout.at[:, cols(owner, 2 * i + d)]
        return remote(part, part, wf_s.at[d, i], wf_r.at[d, i], "samp", ring[d])

    def w_local(k):
        return pltpu.make_async_copy(wbuf.at[k], wout.at[:, cols(y, k)], wl_sem.at[k])

    def each(count, body):
        lax.fori_loop(0, count, lambda i, c: (body(i), c)[1], 0)

    def start_local(k):
        own_copy(k).start()
        w_load(k).start()
        e_load(k).start()

    for k in range(V_SLOTS):
        for copy in v_load(k, k):
            copy.start()

    barrier = pltpu.get_barrier_semaphore()
    for o in range(1, ns):
        pl.semaphore_signal(barrier, inc=1, device_id={"samp": lax.rem(y + o, ns)}, device_id_type=MESH)
    for o in range(1, nf):
        pl.semaphore_signal(barrier, inc=1, device_id={"feat": lax.rem(f + o, nf)}, device_id_type=MESH)
    pl.semaphore_wait(barrier, ns - 1 + nf - 1)

    def start_relay(i):
        for d in range(2):
            relay_copy(d, i).start()

    each(half, start_relay)

    def v_step(k, acc):
        slot = lax.rem(k, V_SLOTS)
        for copy in v_load(k, slot):
            copy.wait()
        low = vw[slot].astype(jnp.bfloat16)
        acc = acc + lax.dot_general(low, vx[slot], NT, preferred_element_type=jnp.float32)

        @pl.when(k + V_SLOTS < v_steps)
        def _():
            for copy in v_load(k + V_SLOTS, slot):
                copy.start()

        return acc

    first = lax.fori_loop(0, v_steps, v_step, jnp.zeros((targets, rows), jnp.float32))
    each(CHUNKS, start_local)

    def a_copy(t, o, place):
        to = lax.rem(y + o, ns)
        return remote(usend.at[t, to], rsbuf.at[t, place], a_s.at[t, o - 1], a_r.at[t, o - 1], "samp", to)

    def b_copy(t, o, place):
        return remote(agbuf.at[t, f], agbuf.at[t, place], b_s.at[t, o - 1], b_r.at[t, o - 1], "feat", lax.rem(f + o, nf))

    def c_copy(t, o, place):
        return remote(rbuf.at[t, y], rbuf.at[t, place], c_s.at[t, o - 1], c_r.at[t, o - 1], "samp", lax.rem(y + o, ns))

    def start_a(t, u):
        for s in range(ns):
            usend[t, s] = u[:, s * rows:(s + 1) * rows]
        for o in range(1, ns):
            a_copy(t, o, y).start()
        rsbuf[t, y] = usend[t, y]

    def finish_a(t):
        for o in range(1, ns):
            a_copy(t, o, lax.rem(y + ns - o, ns)).wait_recv()
        total = rsbuf[t, 0]
        for s in range(1, ns):
            total = total + rsbuf[t, s]
        return total

    def sum_blocks(t, term):
        agbuf[t, f] = term.astype(jnp.bfloat16)
        for o in range(1, nf):
            b_copy(t, o, f).start()
        for o in range(1, nf):
            b_copy(t, o, lax.rem(f + nf - o, nf)).wait_recv()
        total = agbuf[t, 0].astype(jnp.float32)
        for j in range(1, nf):
            total = total + agbuf[t, j].astype(jnp.float32)
        return total

    def start_c(t):
        rbuf[t, y] = rstate[...].astype(jnp.bfloat16)
        for o in range(1, ns):
            c_copy(t, o, y).start()

    def finish_c(t):
        for o in range(1, ns):
            c_copy(t, o, lax.rem(y + ns - o, ns)).wait_recv()
        return jnp.concatenate([rbuf[t, s] for s in range(ns)], axis=1)

    rstate[...] = yt_ref[...] - sum_blocks(0, first)
    start_c(0)

    def start_direct(k):
        for d in range(2):
            direct_copy(d, k, y).start()

    each(CHUNKS, start_direct)

    def start_forward(i):
        for d in range(2):
            relay_copy(d, i).wait_recv()
            forward_copy(d, i, ring[1 - d]).start()

    each(half, start_forward)

    def sweep_chunk(k, resid, u):
        for s in range(chunk // sub):
            part = pl.ds(s * sub, sub)
            x_part = xbuf[k, :, part]
            grad = jnp.dot(resid, x_part, preferred_element_type=jnp.float32) * inv
            w_part = wbuf[k, :, part]
            delta = ebuf[k, :, part] * (grad - ridge * w_part)
            wbuf[k, :, part] = w_part + COMBINE_WEIGHT * delta
            u = u + lax.dot_general(delta.astype(jnp.bfloat16), x_part, NT, preferred_element_type=jnp.float32)
        return u

    zero = jnp.zeros((targets, samples), jnp.float32)

    def arriving(i, carry):
        resid, u = carry
        for d in range(2):
            k = 2 * i + d
            own_copy(k).wait()
            w_load(k).wait()
            e_load(k).wait()
            for e in range(2):
                direct_copy(e, k, ring[1 - e]).wait_recv()
            forward_copy(d, i, far).wait_recv()
            u = sweep_chunk(k, resid, u)
        return resid, u

    def staying(k, carry):
        resid, u = carry
        return resid, sweep_chunk(k, resid, u)

    def send_w(k):
        for d in range(2):
            wd_copy(d, k, y).start()
        w_local(k).start()

    def leaving(k, carry):
        resid, u = carry
        u = sweep_chunk(k, resid, u)

        @pl.when(k > 0)
        def _():
            send_w(k - 1)

        return resid, u

    for t in range(SWEEPS):
        resid = finish_c(t)
        if t == 0:
            _, u = lax.fori_loop(0, half, arriving, (resid, zero))
        elif t < SWEEPS - 1:
            _, u = lax.fori_loop(0, CHUNKS, staying, (resid, zero))
        else:
            _, u = lax.fori_loop(0, CHUNKS, leaving, (resid, zero))
        start_a(t, u)
        if t < SWEEPS - 1:
            rstate[...] = rstate[...] - COMBINE_WEIGHT * sum_blocks(t + 1, finish_a(t))
            start_c(t + 1)

    send_w(CHUNKS - 1)

    def start_wf(i):
        for d in range(2):
            k = 2 * i + d
            for e in range(2):
                wd_copy(e, k, ring[1 - e]).wait_recv()
            wf_copy(d, i, ring[1 - d]).start()

    def start_wf_pair(i):
        start_wf(i)

    each(half, start_wf_pair)
    rout[...] = rstate[...] - COMBINE_WEIGHT * sum_blocks(SWEEPS, finish_a(SWEEPS - 1))

    def finish_half(i):
        for d in range(2):
            relay_copy(d, i).wait_send()
            forward_copy(d, i, ring[1 - d]).wait_send()
            wf_copy(d, i, far).wait_recv()
            wf_copy(d, i, ring[1 - d]).wait_send()

    def finish_full(k):
        for d in range(2):
            direct_copy(d, k, y).wait_send()
            wd_copy(d, k, y).wait_send()
        w_local(k).wait()

    each(CHUNKS, finish_full)
    each(half, finish_half)
    for t in range(SWEEPS):
        for o in range(1, ns):
            a_copy(t, o, y).wait_send()
            c_copy(t, o, y).wait_send()
    for t in range(SWEEPS + 1):
        for o in range(1, nf):
            b_copy(t, o, f).wait_send()


def solution(mesh):
    ns, nf = mesh.shape["samp"], mesh.shape["feat"]

    def local_solve(x_loc, w_loc, y_loc, eta_loc):
        rows, feat_len = x_loc.shape
        targets = w_loc.shape[1]
        samples = rows * ns
        chunk = feat_len // ns // CHUNKS
        half = CHUNKS // 2
        dma = pltpu.SemaphoreType.DMA
        hbm = pl.BlockSpec(memory_space=pl.ANY)
        vmem = pl.BlockSpec(memory_space=pltpu.VMEM)
        small = feat_len * targets
        w_out, r_out = pl.pallas_call(
            functools.partial(kernel, ns, nf),
            out_shape=(jax.ShapeDtypeStruct((targets, feat_len), jnp.float32), jax.ShapeDtypeStruct((targets, rows), jnp.float32)),
            in_specs=[hbm, hbm, vmem, hbm],
            out_specs=(hbm, vmem),
            scratch_shapes=[
                pltpu.VMEM((CHUNKS, samples, chunk), jnp.bfloat16),
                pltpu.VMEM((2, half, rows, chunk), jnp.bfloat16),
                pltpu.VMEM((CHUNKS, targets, chunk), jnp.float32),
                pltpu.VMEM((CHUNKS, 1, chunk), jnp.float32),
                pltpu.VMEM((V_SLOTS, rows, chunk), jnp.bfloat16),
                pltpu.VMEM((V_SLOTS, targets, chunk), jnp.float32),
                pltpu.VMEM((SWEEPS, ns, targets, rows), jnp.float32),
                pltpu.VMEM((SWEEPS, ns, targets, rows), jnp.float32),
                pltpu.VMEM((SWEEPS + 1, nf, targets, rows), jnp.bfloat16),
                pltpu.VMEM((SWEEPS, ns, targets, rows), jnp.bfloat16),
                pltpu.VMEM((targets, rows), jnp.float32),
                dma((CHUNKS,)), dma((CHUNKS,)), dma((CHUNKS,)), dma((2, V_SLOTS)),
                dma((2, half)), dma((2, half)), dma((2, CHUNKS)), dma((2, CHUNKS)), dma((2, half)), dma((2, half)),
                dma((SWEEPS, ns - 1)), dma((SWEEPS, ns - 1)),
                dma((SWEEPS + 1, nf - 1)), dma((SWEEPS + 1, nf - 1)),
                dma((SWEEPS, ns - 1)), dma((SWEEPS, ns - 1)),
                dma((CHUNKS,)), dma((2, CHUNKS)), dma((2, CHUNKS)), dma((2, half)), dma((2, half)),
            ],
            compiler_params=pltpu.CompilerParams(collective_id=0, has_side_effects=True, vmem_limit_bytes=64 * 1024 * 1024 - 256 * 1024),
            cost_estimate=pl.CostEstimate(flops=2 * rows * small * (2 * SWEEPS + 1), bytes_accessed=8 * small + 4 * rows * feat_len,
                                          transcendentals=0),
            name="ridge_sweeps",
        )(x_loc, w_loc.T, y_loc.T, eta_loc.reshape(1, feat_len))
        return w_out.T, r_out.T

    return jax.shard_map(
        local_solve,
        mesh=mesh,
        in_specs=(P(("prob", "samp"), "feat"), P(("prob", "feat"), None), P(("prob", "samp"), None), P(("prob", "feat"))),
        out_specs=(P(("prob", "feat"), None), P(("prob", "samp"), None)),
        check_vma=False,
    )
```

```python
import functools

import jax
import jax.numpy as jnp
from jax import lax
from jax.experimental import pallas as pl
from jax.experimental.pallas import tpu as pltpu
from jax.sharding import PartitionSpec as P

SWEEPS = 4
COMBINE_WEIGHT = 0.8
RIDGE_SCALE = 0.1
CHUNKS = 16
SUB = 512
STREAM = 0.5
V_SLOTS = 4
MESH = pl.DeviceIdType.MESH
NT = (((1,), (1,)), ((), ()))


def far_first(count):
    return sorted(range(1, count), key=lambda o: -min(o, count - o))


def kernel(ns, nf, x_hbm, wt_hbm, yt_ref, eta_hbm, wout, rout, xbuf, relay, ebuf, vx, vw, usend, rsbuf, agbuf, rbuf, rstate, ucol, urow,
           own_sem, w_sem, e_sem, v_sem, rel_s, rel_r, dir_s, dir_r, fwd_s, fwd_r, a_s, a_r, b_s, b_r, c_s, c_r,
           wd_s, wd_r, wf_s, wf_r):
    y, f = lax.axis_index("samp"), lax.axis_index("feat")
    rows, feat_len = x_hbm.shape
    targets = wt_hbm.shape[0]
    own = feat_len // ns
    chunk = own // CHUNKS
    half = CHUNKS // 2
    sub = min(SUB, chunk)
    samples = rows * ns
    inv = 1.0 / samples
    ridge = RIDGE_SCALE * (feat_len * nf) / samples
    up, down, far = lax.rem(y + 1, ns), lax.rem(y + ns - 1, ns), lax.rem(y + 2, ns)
    ring = (up, down)

    def cols(owner, k):
        return pl.ds(pl.multiple_of(owner * own + k * chunk, chunk), chunk)

    def rows_of(s):
        return pl.ds(pl.multiple_of(s * rows, rows), rows)

    def remote(src, dst, send, recv, axis, dev):
        return pltpu.make_async_remote_copy(src_ref=src, dst_ref=dst, send_sem=send, recv_sem=recv,
                                            device_id={axis: dev}, device_id_type=MESH)

    def own_copy(k):
        return pltpu.make_async_copy(x_hbm.at[:, cols(y, k)], xbuf.at[k, rows_of(y), :], own_sem.at[k])

    def w_load(k):
        return pltpu.make_async_copy(wt_hbm.at[:, cols(y, k)], wout.at[:, cols(y, k)], w_sem.at[k])

    def e_load(k):
        return pltpu.make_async_copy(eta_hbm.at[:, cols(y, k)], ebuf.at[k], e_sem.at[k])

    v_steps = ns * CHUNKS

    def v_cols(k):
        return pl.ds(pl.multiple_of(k * chunk, chunk), chunk)

    def v_load(k, slot):
        return (pltpu.make_async_copy(x_hbm.at[:, v_cols(k)], vx.at[slot], v_sem.at[0, slot]),
                pltpu.make_async_copy(wt_hbm.at[:, v_cols(k)], vw.at[slot], v_sem.at[1, slot]))

    def relay_copy(d, i):
        return remote(x_hbm.at[:, cols(far, 2 * i + d)], relay.at[d, i], rel_s.at[d, i], rel_r.at[d, i], "samp", ring[d])

    def direct_copy(d, k, place):
        return remote(x_hbm.at[:, cols(ring[d], k)], xbuf.at[k, rows_of(place), :], dir_s.at[d, k], dir_r.at[d, k], "samp", ring[d])

    def forward_copy(d, i, place):
        return remote(relay.at[d, i], xbuf.at[2 * i + d, rows_of(place), :], fwd_s.at[d, i], fwd_r.at[d, i], "samp", ring[d])

    def wd_copy(d, k, owner):
        return remote(wout.at[:, cols(y, k)], wout.at[:, cols(owner, k)], wd_s.at[d, k], wd_r.at[d, k], "samp", ring[d])

    def wf_copy(d, i, owner):
        part = wout.at[:, cols(owner, 2 * i + d)]
        return remote(part, part, wf_s.at[d, i], wf_r.at[d, i], "samp", ring[d])

    def each(count, body):
        lax.fori_loop(0, count, lambda i, c: (body(i), c)[1], 0)

    def start_local(k):
        own_copy(k).start()
        w_load(k).start()
        e_load(k).start()

    for k in range(V_SLOTS):
        for copy in v_load(k, k):
            copy.start()

    barrier = pltpu.get_barrier_semaphore()
    for o in range(1, ns):
        pl.semaphore_signal(barrier, inc=1, device_id={"samp": lax.rem(y + o, ns)}, device_id_type=MESH)
    for o in range(1, nf):
        pl.semaphore_signal(barrier, inc=1, device_id={"feat": lax.rem(f + o, nf)}, device_id_type=MESH)
    pl.semaphore_wait(barrier, ns - 1 + nf - 1)

    def start_relay(i):
        for d in range(2):
            relay_copy(d, i).start()

    each(half, start_relay)

    def v_step(k, acc):
        slot = lax.rem(k, V_SLOTS)
        for copy in v_load(k, slot):
            copy.wait()
        low = vw[slot].astype(jnp.bfloat16)
        acc = acc + lax.dot_general(low, vx[slot], NT, preferred_element_type=jnp.float32)

        @pl.when(k + V_SLOTS < v_steps)
        def _():
            for copy in v_load(k + V_SLOTS, slot):
                copy.start()

        return acc

    first = lax.fori_loop(0, v_steps, v_step, jnp.zeros((targets, rows), jnp.float32))
    each(CHUNKS, start_local)

    def a_copy(t, o, place):
        to = lax.rem(y + o, ns)
        return remote(usend.at[t, to], rsbuf.at[t, place], a_s.at[t, o - 1], a_r.at[t, o - 1], "samp", to)

    def b_copy(t, o, place):
        return remote(agbuf.at[t, f], agbuf.at[t, place], b_s.at[t, o - 1], b_r.at[t, o - 1], "feat", lax.rem(f + o, nf))

    def c_copy(t, o, place):
        return remote(rbuf.at[t, y], rbuf.at[t, place], c_s.at[t, o - 1], c_r.at[t, o - 1], "samp", lax.rem(y + o, ns))

    def start_a(t):
        for s in range(ns):
            usend[t, s] = ucol[s * rows:(s + 1) * rows, :].T + urow[:, s * rows:(s + 1) * rows]
        for o in far_first(ns):
            a_copy(t, o, y).start()
        rsbuf[t, y] = usend[t, y]

    def finish_a(t):
        for o in range(1, ns):
            a_copy(t, o, lax.rem(y + ns - o, ns)).wait_recv()
        total = rsbuf[t, 0]
        for s in range(1, ns):
            total = total + rsbuf[t, s]
        return total

    def sum_blocks(t, term):
        agbuf[t, f] = term.astype(jnp.bfloat16)
        for o in far_first(nf):
            b_copy(t, o, f).start()
        for o in range(1, nf):
            b_copy(t, o, lax.rem(f + nf - o, nf)).wait_recv()
        total = agbuf[t, 0].astype(jnp.float32)
        for j in range(1, nf):
            total = total + agbuf[t, j].astype(jnp.float32)
        return total

    def start_c(t):
        rbuf[t, y] = rstate[...].astype(jnp.bfloat16)
        for o in far_first(ns):
            c_copy(t, o, y).start()

    def finish_c(t):
        for o in range(1, ns):
            c_copy(t, o, lax.rem(y + ns - o, ns)).wait_recv()
        return jnp.concatenate([rbuf[t, s] for s in range(ns)], axis=1)

    rstate[...] = yt_ref[...] - sum_blocks(0, first)
    start_c(0)

    def start_direct(k):
        for d in range(2):
            direct_copy(d, k, y).start()

    each(CHUNKS, start_direct)

    def start_forward(i):
        for d in range(2):
            relay_copy(d, i).wait_recv()
            forward_copy(d, i, ring[1 - d]).start()

    each(half, start_forward)

    def sweep_chunk(k, resid):
        parts = chunk // sub
        col, row = None, None
        for s in range(parts):
            part = pl.ds(s * sub, sub)
            x_part = xbuf[k, :, part]
            grad = jnp.dot(resid, x_part, preferred_element_type=jnp.float32) * inv
            place = pl.ds(pl.multiple_of(y * own + k * chunk + s * sub, sub), sub)
            w_part = wout[:, place]
            delta = ebuf[k, :, part] * (grad - ridge * w_part)
            wout[:, place] = w_part + COMBINE_WEIGHT * delta
            low = delta.astype(jnp.bfloat16)
            if s < STREAM * parts:
                term = lax.dot_general(x_part, low, NT, preferred_element_type=jnp.float32)
                col = term if col is None else col + term
            else:
                term = lax.dot_general(low, x_part, NT, preferred_element_type=jnp.float32)
                row = term if row is None else row + term
        if col is not None:
            ucol[...] += col
        if row is not None:
            urow[...] += row

    def arriving(i):
        for d in range(2):
            k = 2 * i + d
            own_copy(k).wait()
            w_load(k).wait()
            e_load(k).wait()
            for e in range(2):
                direct_copy(e, k, ring[1 - e]).wait_recv()
            forward_copy(d, i, far).wait_recv()
            sweep_chunk(k, resid)

    def staying(k):
        sweep_chunk(k, resid)

    def send_w(k):
        for d in range(2):
            wd_copy(d, k, y).start()

    def leaving(k):
        sweep_chunk(k, resid)

        @pl.when(k > 0)
        def _():
            send_w(k - 1)

    for t in range(SWEEPS):
        resid = finish_c(t)
        ucol[...] = jnp.zeros_like(ucol)
        urow[...] = jnp.zeros_like(urow)
        if t == 0:
            each(half, arriving)
        elif t < SWEEPS - 1:
            each(CHUNKS, staying)
        else:
            each(CHUNKS, leaving)
        start_a(t)
        if t < SWEEPS - 1:
            rstate[...] = rstate[...] - COMBINE_WEIGHT * sum_blocks(t + 1, finish_a(t))
            start_c(t + 1)

    send_w(CHUNKS - 1)

    def start_wf(i):
        for d in range(2):
            k = 2 * i + d
            for e in range(2):
                wd_copy(e, k, ring[1 - e]).wait_recv()
            wf_copy(d, i, ring[1 - d]).start()

    def start_wf_pair(i):
        start_wf(i)

    each(half, start_wf_pair)
    rout[...] = rstate[...] - COMBINE_WEIGHT * sum_blocks(SWEEPS, finish_a(SWEEPS - 1))

    def finish_half(i):
        for d in range(2):
            relay_copy(d, i).wait_send()
            forward_copy(d, i, ring[1 - d]).wait_send()
            wf_copy(d, i, far).wait_recv()
            wf_copy(d, i, ring[1 - d]).wait_send()

    def finish_full(k):
        for d in range(2):
            direct_copy(d, k, y).wait_send()
            wd_copy(d, k, y).wait_send()

    each(CHUNKS, finish_full)
    each(half, finish_half)
    for t in range(SWEEPS):
        for o in range(1, ns):
            a_copy(t, o, y).wait_send()
            c_copy(t, o, y).wait_send()
    for t in range(SWEEPS + 1):
        for o in range(1, nf):
            b_copy(t, o, f).wait_send()


def solution(mesh):
    ns, nf = mesh.shape["samp"], mesh.shape["feat"]

    def local_solve(x_loc, w_loc, y_loc, eta_loc):
        rows, feat_len = x_loc.shape
        targets = w_loc.shape[1]
        samples = rows * ns
        chunk = feat_len // ns // CHUNKS
        half = CHUNKS // 2
        dma = pltpu.SemaphoreType.DMA
        hbm = pl.BlockSpec(memory_space=pl.ANY)
        vmem = pl.BlockSpec(memory_space=pltpu.VMEM)
        small = feat_len * targets
        w_out, r_out = pl.pallas_call(
            functools.partial(kernel, ns, nf),
            out_shape=(pltpu.VMEM((targets, feat_len), jnp.float32), pltpu.VMEM((targets, rows), jnp.float32)),
            in_specs=[hbm, hbm, vmem, hbm],
            out_specs=(vmem, vmem),
            scratch_shapes=[
                pltpu.VMEM((CHUNKS, samples, chunk), jnp.bfloat16),
                pltpu.VMEM((2, half, rows, chunk), jnp.bfloat16),
                pltpu.VMEM((CHUNKS, 1, chunk), jnp.float32),
                pltpu.VMEM((V_SLOTS, rows, chunk), jnp.bfloat16),
                pltpu.VMEM((V_SLOTS, targets, chunk), jnp.float32),
                pltpu.VMEM((SWEEPS, ns, targets, rows), jnp.float32),
                pltpu.VMEM((SWEEPS, ns, targets, rows), jnp.float32),
                pltpu.VMEM((SWEEPS + 1, nf, targets, rows), jnp.bfloat16),
                pltpu.VMEM((SWEEPS, ns, targets, rows), jnp.bfloat16),
                pltpu.VMEM((targets, rows), jnp.float32),
                pltpu.VMEM((samples, targets), jnp.float32),
                pltpu.VMEM((targets, samples), jnp.float32),
                dma((CHUNKS,)), dma((CHUNKS,)), dma((CHUNKS,)), dma((2, V_SLOTS)),
                dma((2, half)), dma((2, half)), dma((2, CHUNKS)), dma((2, CHUNKS)), dma((2, half)), dma((2, half)),
                dma((SWEEPS, ns - 1)), dma((SWEEPS, ns - 1)),
                dma((SWEEPS + 1, nf - 1)), dma((SWEEPS + 1, nf - 1)),
                dma((SWEEPS, ns - 1)), dma((SWEEPS, ns - 1)),
                dma((2, CHUNKS)), dma((2, CHUNKS)), dma((2, half)), dma((2, half)),
            ],
            compiler_params=pltpu.CompilerParams(collective_id=0, has_side_effects=True, vmem_limit_bytes=47 * 1024 * 1024),
            cost_estimate=pl.CostEstimate(flops=2 * rows * small * (2 * SWEEPS + 1), bytes_accessed=8 * small + 4 * rows * feat_len,
                                          transcendentals=0),
            name="ridge_sweeps",
        )(x_loc, w_loc.T, y_loc.T, eta_loc.reshape(1, feat_len))
        return w_out.T, r_out.T

    return jax.shard_map(
        local_solve,
        mesh=mesh,
        in_specs=(P(("prob", "samp"), "feat"), P(("prob", "feat"), None), P(("prob", "samp"), None), P(("prob", "feat"))),
        out_specs=(P(("prob", "feat"), None), P(("prob", "samp"), None)),
        check_vma=False,
    )
```

```python
import functools

import jax
import jax.numpy as jnp
from jax import lax
from jax.experimental import pallas as pl
from jax.experimental.pallas import tpu as pltpu
from jax.sharding import PartitionSpec as P

SWEEPS = 4
COMBINE_WEIGHT = 0.8
RIDGE_SCALE = 0.1
CHUNKS = 16
SUB = 512
STREAM = 0.5
V_SLOTS = 3
MESH = pl.DeviceIdType.MESH
NT = (((1,), (1,)), ((), ()))


def far_first(count):
    return sorted(range(1, count), key=lambda o: -min(o, count - o))


def kernel(ns, nf, x_hbm, wt_hbm, yt_ref, eta_hbm, wout, rout, xbuf, relay, dbuf, ebuf, vx, vw, usend, rsbuf, agbuf, rbuf, rstate, ucol, urow,
           own_sem, w_sem, e_sem, v_sem, rel_s, rel_r, dir_s, dir_r, fwd_s, fwd_r, a_s, a_r, b_s, b_r, c_s, c_r,
           wd_s, wd_r, wf_s, wf_r):
    y, f = lax.axis_index("samp"), lax.axis_index("feat")
    rows, feat_len = x_hbm.shape
    targets = wt_hbm.shape[0]
    own = feat_len // ns
    chunk = own // CHUNKS
    half = CHUNKS // 2
    sub = min(SUB, chunk)
    samples = rows * ns
    inv = 1.0 / samples
    ridge = RIDGE_SCALE * (feat_len * nf) / samples
    up, down, far = lax.rem(y + 1, ns), lax.rem(y + ns - 1, ns), lax.rem(y + 2, ns)
    ring = (up, down)

    def cols(owner, k):
        return pl.ds(pl.multiple_of(owner * own + k * chunk, chunk), chunk)

    def rows_of(o):
        return pl.ds(o * rows, rows)

    def remote(src, dst, send, recv, axis, dev):
        return pltpu.make_async_remote_copy(src_ref=src, dst_ref=dst, send_sem=send, recv_sem=recv,
                                            device_id={axis: dev}, device_id_type=MESH)

    def own_copy(k):
        return pltpu.make_async_copy(x_hbm.at[:, cols(y, k)], xbuf.at[k, rows_of(0), :], own_sem.at[k])

    def w_load(k):
        return pltpu.make_async_copy(wt_hbm.at[:, cols(y, k)], wout.at[:, cols(y, k)], w_sem.at[k])

    def e_load(k):
        return pltpu.make_async_copy(eta_hbm.at[:, cols(y, k)], ebuf.at[k], e_sem.at[k])

    v_steps = ns * CHUNKS

    def v_cols(k):
        return pl.ds(pl.multiple_of(k * chunk, chunk), chunk)

    def v_load(k, slot):
        return (pltpu.make_async_copy(x_hbm.at[:, v_cols(k)], vx.at[slot], v_sem.at[0, slot]),
                pltpu.make_async_copy(wt_hbm.at[:, v_cols(k)], vw.at[slot], v_sem.at[1, slot]))

    def relay_copy(d, i):
        return remote(x_hbm.at[:, cols(far, 2 * i + d)], relay.at[d, i], rel_s.at[d, i], rel_r.at[d, i], "samp", ring[d])

    def direct_copy(d, k):
        return remote(x_hbm.at[:, cols(ring[d], k)], xbuf.at[k, rows_of((ns - 1, 1)[d]), :], dir_s.at[d, k], dir_r.at[d, k], "samp", ring[d])

    def forward_copy(d, i):
        return remote(relay.at[d, i], xbuf.at[2 * i + d, rows_of(2), :], fwd_s.at[d, i], fwd_r.at[d, i], "samp", ring[d])

    def wd_copy(d, k, owner):
        return remote(wout.at[:, cols(y, k)], wout.at[:, cols(owner, k)], wd_s.at[d, k], wd_r.at[d, k], "samp", ring[d])

    def wf_copy(d, i, owner):
        part = wout.at[:, cols(owner, 2 * i + d)]
        return remote(part, part, wf_s.at[d, i], wf_r.at[d, i], "samp", ring[d])

    def each(count, body):
        lax.fori_loop(0, count, lambda i, c: (body(i), c)[1], 0)

    def start_local(k):
        own_copy(k).start()
        w_load(k).start()
        e_load(k).start()

    for k in range(V_SLOTS):
        for copy in v_load(k, k):
            copy.start()

    barrier = pltpu.get_barrier_semaphore()
    for o in range(1, ns):
        pl.semaphore_signal(barrier, inc=1, device_id={"samp": lax.rem(y + o, ns)}, device_id_type=MESH)
    for o in range(1, nf):
        pl.semaphore_signal(barrier, inc=1, device_id={"feat": lax.rem(f + o, nf)}, device_id_type=MESH)
    pl.semaphore_wait(barrier, ns - 1 + nf - 1)

    def start_relay(i):
        for d in range(2):
            relay_copy(d, i).start()

    each(half, start_relay)

    def v_step(k, acc):
        slot = lax.rem(k, V_SLOTS)
        for copy in v_load(k, slot):
            copy.wait()
        low = vw[slot].astype(jnp.bfloat16)
        acc = acc + lax.dot_general(low, vx[slot], NT, preferred_element_type=jnp.float32)

        @pl.when(k + V_SLOTS < v_steps)
        def _():
            for copy in v_load(k + V_SLOTS, slot):
                copy.start()

        return acc

    first = lax.fori_loop(0, v_steps, v_step, jnp.zeros((targets, rows), jnp.float32))
    each(CHUNKS, start_local)

    def a_copy(t, o):
        return remote(usend.at[t, o], rsbuf.at[t, ns - o], a_s.at[t, o - 1], a_r.at[t, o - 1], "samp", lax.rem(y + o, ns))

    def b_copy(t, o, place):
        return remote(agbuf.at[t, f], agbuf.at[t, place], b_s.at[t, o - 1], b_r.at[t, o - 1], "feat", lax.rem(f + o, nf))

    def c_copy(t, o):
        return remote(rbuf.at[t, 0], rbuf.at[t, ns - o], c_s.at[t, o - 1], c_r.at[t, o - 1], "samp", lax.rem(y + o, ns))

    def start_a(t):
        for o in range(1, ns):
            usend[t, o] = ucol[(o - 1) * rows:o * rows, :].T + urow[:, (o - 1) * rows:o * rows]
        for o in far_first(ns):
            a_copy(t, o).start()

    def finish_a(t, total):
        for o in range(1, ns):
            a_copy(t, o).wait_recv()
        for o in range(1, ns):
            total = total + rsbuf[t, o]
        return total

    def sum_blocks(t, term):
        agbuf[t, f] = term.astype(jnp.bfloat16)
        for o in far_first(nf):
            b_copy(t, o, f).start()
        for o in range(1, nf):
            b_copy(t, o, lax.rem(f + nf - o, nf)).wait_recv()
        total = agbuf[t, 0].astype(jnp.float32)
        for j in range(1, nf):
            total = total + agbuf[t, j].astype(jnp.float32)
        return total

    def start_c(t):
        rbuf[t, 0] = rstate[...].astype(jnp.bfloat16)
        for o in far_first(ns):
            c_copy(t, o).start()

    def finish_c(t):
        for o in range(1, ns):
            c_copy(t, o).wait_recv()
        return jnp.concatenate([rbuf[t, o] for o in range(ns)], axis=1)

    rstate[...] = yt_ref[...] - sum_blocks(0, first)
    start_c(0)

    def start_direct(k):
        for d in range(2):
            direct_copy(d, k).start()

    each(CHUNKS, start_direct)

    def start_forward(i):
        for d in range(2):
            relay_copy(d, i).wait_recv()
            forward_copy(d, i).start()

    each(half, start_forward)

    parts = chunk // sub

    def advance(k, s, resid):
        part = pl.ds(s * sub, sub)
        grad = jnp.dot(resid, xbuf[k, :, part], preferred_element_type=jnp.float32) * inv
        place = pl.ds(pl.multiple_of(y * own + k * chunk + s * sub, sub), sub)
        w_part = wout[:, place]
        delta = ebuf[k, :, part] * (grad - ridge * w_part)
        wout[:, place] = w_part + COMBINE_WEIGHT * delta
        low = delta.astype(jnp.bfloat16)
        dbuf[k, :, part] = low
        return low

    def other_rows(k, low_of):
        col, row = None, None
        for s in range(parts):
            low = low_of(s)
            x_part = xbuf[k, rows:, pl.ds(s * sub, sub)]
            if s < STREAM * parts:
                term = lax.dot_general(x_part, low, NT, preferred_element_type=jnp.float32)
                col = term if col is None else col + term
            else:
                term = lax.dot_general(low, x_part, NT, preferred_element_type=jnp.float32)
                row = term if row is None else row + term
        if col is not None:
            ucol[...] += col
        if row is not None:
            urow[...] += row

    def sweep_chunk(k, resid):
        other_rows(k, lambda s: advance(k, s, resid))

    def own_rows(k, acc):
        return acc + lax.dot_general(xbuf[k, :rows, :], dbuf[k], NT, preferred_element_type=jnp.float32)

    def arriving(i):
        for d in range(2):
            k = 2 * i + d
            own_copy(k).wait()
            w_load(k).wait()
            e_load(k).wait()
            for e in range(2):
                direct_copy(e, k).wait_recv()
            forward_copy(d, i).wait_recv()
            sweep_chunk(k, resid)

    def from_store(k):
        other_rows(k, lambda s: dbuf[k, :, pl.ds(s * sub, sub)])

    def staying(k):
        for s in range(parts):
            advance(k, s, resid)

    def send_w(k):
        for d in range(2):
            wd_copy(d, k, y).start()

    def leaving(k):
        for s in range(parts):
            advance(k, s, resid)

        @pl.when(k > 0)
        def _():
            send_w(k - 1)

    for t in range(SWEEPS):
        resid = finish_c(t)
        ucol[...] = jnp.zeros_like(ucol)
        urow[...] = jnp.zeros_like(urow)
        if t == 0:
            each(half, arriving)
        elif t < SWEEPS - 1:
            each(CHUNKS, staying)
            each(CHUNKS, from_store)
        else:
            each(CHUNKS, leaving)
            send_w(CHUNKS - 1)
            each(CHUNKS, from_store)
        start_a(t)
        mine = lax.fori_loop(0, CHUNKS, own_rows, jnp.zeros((rows, targets), jnp.float32)).T
        if t < SWEEPS - 1:
            rstate[...] = rstate[...] - COMBINE_WEIGHT * sum_blocks(t + 1, finish_a(t, mine))
            start_c(t + 1)

    def start_wf(i):
        for d in range(2):
            k = 2 * i + d
            for e in range(2):
                wd_copy(e, k, ring[1 - e]).wait_recv()
            wf_copy(d, i, ring[1 - d]).start()

    def start_wf_pair(i):
        start_wf(i)

    each(half, start_wf_pair)
    rout[...] = rstate[...] - COMBINE_WEIGHT * sum_blocks(SWEEPS, finish_a(SWEEPS - 1, mine))

    def finish_half(i):
        for d in range(2):
            relay_copy(d, i).wait_send()
            forward_copy(d, i).wait_send()
            wf_copy(d, i, far).wait_recv()
            wf_copy(d, i, ring[1 - d]).wait_send()

    def finish_full(k):
        for d in range(2):
            direct_copy(d, k).wait_send()
            wd_copy(d, k, y).wait_send()

    each(CHUNKS, finish_full)
    each(half, finish_half)
    for t in range(SWEEPS):
        for o in range(1, ns):
            a_copy(t, o).wait_send()
            c_copy(t, o).wait_send()
    for t in range(SWEEPS + 1):
        for o in range(1, nf):
            b_copy(t, o, f).wait_send()


def solution(mesh):
    ns, nf = mesh.shape["samp"], mesh.shape["feat"]

    def local_solve(x_loc, w_loc, y_loc, eta_loc):
        rows, feat_len = x_loc.shape
        targets = w_loc.shape[1]
        samples = rows * ns
        chunk = feat_len // ns // CHUNKS
        half = CHUNKS // 2
        dma = pltpu.SemaphoreType.DMA
        hbm = pl.BlockSpec(memory_space=pl.ANY)
        vmem = pl.BlockSpec(memory_space=pltpu.VMEM)
        small = feat_len * targets
        w_out, r_out = pl.pallas_call(
            functools.partial(kernel, ns, nf),
            out_shape=(pltpu.VMEM((targets, feat_len), jnp.float32), pltpu.VMEM((targets, rows), jnp.float32)),
            in_specs=[hbm, hbm, vmem, hbm],
            out_specs=(vmem, vmem),
            scratch_shapes=[
                pltpu.VMEM((CHUNKS, samples, chunk), jnp.bfloat16),
                pltpu.VMEM((2, half, rows, chunk), jnp.bfloat16),
                pltpu.VMEM((CHUNKS, targets, chunk), jnp.bfloat16),
                pltpu.VMEM((CHUNKS, 1, chunk), jnp.float32),
                pltpu.VMEM((V_SLOTS, rows, chunk), jnp.bfloat16),
                pltpu.VMEM((V_SLOTS, targets, chunk), jnp.float32),
                pltpu.VMEM((SWEEPS, ns, targets, rows), jnp.float32),
                pltpu.VMEM((SWEEPS, ns, targets, rows), jnp.float32),
                pltpu.VMEM((SWEEPS + 1, nf, targets, rows), jnp.bfloat16),
                pltpu.VMEM((SWEEPS, ns, targets, rows), jnp.bfloat16),
                pltpu.VMEM((targets, rows), jnp.float32),
                pltpu.VMEM((samples - rows, targets), jnp.float32),
                pltpu.VMEM((targets, samples - rows), jnp.float32),
                dma((CHUNKS,)), dma((CHUNKS,)), dma((CHUNKS,)), dma((2, V_SLOTS)),
                dma((2, half)), dma((2, half)), dma((2, CHUNKS)), dma((2, CHUNKS)), dma((2, half)), dma((2, half)),
                dma((SWEEPS, ns - 1)), dma((SWEEPS, ns - 1)),
                dma((SWEEPS + 1, nf - 1)), dma((SWEEPS + 1, nf - 1)),
                dma((SWEEPS, ns - 1)), dma((SWEEPS, ns - 1)),
                dma((2, CHUNKS)), dma((2, CHUNKS)), dma((2, half)), dma((2, half)),
            ],
            compiler_params=pltpu.CompilerParams(collective_id=0, has_side_effects=True, vmem_limit_bytes=47 * 1024 * 1024),
            cost_estimate=pl.CostEstimate(flops=2 * rows * small * (2 * SWEEPS + 1), bytes_accessed=8 * small + 4 * rows * feat_len,
                                          transcendentals=0),
            name="ridge_sweeps",
        )(x_loc, w_loc.T, y_loc.T, eta_loc.reshape(1, feat_len))
        pieces = 8

        def put(w_ref, r_ref, w_hbm, r_hbm, sem):
            width = feat_len // pieces
            copies = [pltpu.make_async_copy(w_ref.at[:, pl.ds(i * width, width)], w_hbm.at[:, pl.ds(i * width, width)], sem.at[i])
                      for i in range(pieces)]
            copies.append(pltpu.make_async_copy(r_ref, r_hbm, sem.at[pieces]))
            for copy in copies:
                copy.start()
            for copy in copies:
                copy.wait()

        w_out, r_out = pl.pallas_call(
            put,
            out_shape=(jax.ShapeDtypeStruct((targets, feat_len), jnp.float32), jax.ShapeDtypeStruct((targets, rows), jnp.float32)),
            in_specs=[vmem, vmem],
            out_specs=(hbm, hbm),
            scratch_shapes=[dma((pieces + 1,))],
            compiler_params=pltpu.CompilerParams(vmem_limit_bytes=1024 * 1024),
            name="put_results",
        )(pltpu.with_memory_space_constraint(w_out, pltpu.VMEM), pltpu.with_memory_space_constraint(r_out, pltpu.VMEM))
        return w_out.T, r_out.T

    return jax.shard_map(
        local_solve,
        mesh=mesh,
        in_specs=(P(("prob", "samp"), "feat"), P(("prob", "feat"), None), P(("prob", "samp"), None), P(("prob", "feat"))),
        out_specs=(P(("prob", "feat"), None), P(("prob", "samp"), None)),
        check_vma=False,
    )
```

```python
import functools

import jax
import jax.numpy as jnp
from jax import lax
from jax.experimental import pallas as pl
from jax.experimental.pallas import tpu as pltpu
from jax.sharding import PartitionSpec as P

SWEEPS = 4
COMBINE_WEIGHT = 0.8
RIDGE_SCALE = 0.1
CHUNKS = 16
SUB = 512
STREAM = 0.5
V_SLOTS = 3
MESH = pl.DeviceIdType.MESH
NT = (((1,), (1,)), ((), ()))


BLOCK = (0, 2, 1, 3)


def far_first(count):
    return sorted(range(1, count), key=lambda o: -min(o, count - o))


def kernel(ns, nf, x_hbm, wt_hbm, yt_ref, eta_hbm, wout, rout, relay, xbuf, gbuf, dbuf, ebuf, vx, vw, usend, rsbuf, agbuf, rbuf, rstate, ucol, urow,
           own_sem, w_sem, e_sem, v_sem, rel_s, rel_r, dir_s, dir_r, fwd_s, fwd_r, a_s, a_r, b_s, b_r, c_s, c_r,
           wd_s, wd_r, wf_s, wf_r):
    y, f = lax.axis_index("samp"), lax.axis_index("feat")
    rows, feat_len = x_hbm.shape
    targets = wt_hbm.shape[0]
    own = feat_len // ns
    chunk = own // CHUNKS
    half = CHUNKS // 2
    sub = min(SUB, chunk)
    samples = rows * ns
    inv = 1.0 / samples
    ridge = RIDGE_SCALE * (feat_len * nf) / samples
    up, down, far = lax.rem(y + 1, ns), lax.rem(y + ns - 1, ns), lax.rem(y + 2, ns)
    ring = (up, down)

    def cols(owner, k):
        return pl.ds(pl.multiple_of(owner * own + k * chunk, chunk), chunk)

    def rows_of(o):
        return pl.ds(BLOCK[o] * rows, rows)

    def remote(src, dst, send, recv, axis, dev):
        return pltpu.make_async_remote_copy(src_ref=src, dst_ref=dst, send_sem=send, recv_sem=recv,
                                            device_id={axis: dev}, device_id_type=MESH)

    def own_copy(k):
        return pltpu.make_async_copy(x_hbm.at[:, cols(y, k)], xbuf.at[k, rows_of(0), :], own_sem.at[k])

    def w_load(k):
        return pltpu.make_async_copy(wt_hbm.at[:, cols(y, k)], wout.at[:, cols(y, k)], w_sem.at[k])

    def e_load(k):
        return pltpu.make_async_copy(eta_hbm.at[:, cols(y, k)], ebuf.at[k], e_sem.at[k])

    v_steps = ns * CHUNKS

    def v_cols(k):
        return pl.ds(pl.multiple_of(k * chunk, chunk), chunk)

    def v_load(k, slot):
        return (pltpu.make_async_copy(x_hbm.at[:, v_cols(k)], vx.at[slot], v_sem.at[0, slot]),
                pltpu.make_async_copy(wt_hbm.at[:, v_cols(k)], vw.at[slot], v_sem.at[1, slot]))

    def relay_copy(d, i):
        return remote(x_hbm.at[:, cols(far, 2 * i + d)], relay.at[d, i], rel_s.at[d, i], rel_r.at[d, i], "samp", ring[d])

    def direct_copy(d, k):
        return remote(x_hbm.at[:, cols(ring[d], k)], xbuf.at[k, rows_of((ns - 1, 1)[d]), :], dir_s.at[d, k], dir_r.at[d, k], "samp", ring[d])

    def forward_copy(d, i):
        return remote(relay.at[d, i], xbuf.at[2 * i + d, rows_of(2), :], fwd_s.at[d, i], fwd_r.at[d, i], "samp", ring[d])

    def wd_copy(d, k, owner):
        return remote(wout.at[:, cols(y, k)], wout.at[:, cols(owner, k)], wd_s.at[d, k], wd_r.at[d, k], "samp", ring[d])

    def wf_copy(d, i, owner):
        part = wout.at[:, cols(owner, 2 * i + d)]
        return remote(part, part, wf_s.at[d, i], wf_r.at[d, i], "samp", ring[d])

    def each(count, body):
        lax.fori_loop(0, count, lambda i, c: (body(i), c)[1], 0)

    def start_local(k):
        own_copy(k).start()
        w_load(k).start()
        e_load(k).start()

    for k in range(V_SLOTS):
        for copy in v_load(k, k):
            copy.start()

    barrier = pltpu.get_barrier_semaphore()
    for o in range(1, ns):
        pl.semaphore_signal(barrier, inc=1, device_id={"samp": lax.rem(y + o, ns)}, device_id_type=MESH)
    for o in range(1, nf):
        pl.semaphore_signal(barrier, inc=1, device_id={"feat": lax.rem(f + o, nf)}, device_id_type=MESH)
    pl.semaphore_wait(barrier, ns - 1 + nf - 1)

    def start_relay(i):
        for d in range(2):
            relay_copy(d, i).start()

    each(half, start_relay)

    def v_step(k, acc):
        slot = lax.rem(k, V_SLOTS)
        for copy in v_load(k, slot):
            copy.wait()
        low = vw[slot].astype(jnp.bfloat16)
        acc = acc + lax.dot_general(low, vx[slot], NT, preferred_element_type=jnp.float32)

        @pl.when(k + V_SLOTS < v_steps)
        def _():
            for copy in v_load(k + V_SLOTS, slot):
                copy.start()

        return acc

    first = lax.fori_loop(0, v_steps, v_step, jnp.zeros((targets, rows), jnp.float32))
    each(CHUNKS, start_local)

    def a_copy(t, o):
        return remote(usend.at[t, o], rsbuf.at[t, ns - o], a_s.at[t, o - 1], a_r.at[t, o - 1], "samp", lax.rem(y + o, ns))

    def b_copy(t, o, place):
        return remote(agbuf.at[t, f], agbuf.at[t, place], b_s.at[t, o - 1], b_r.at[t, o - 1], "feat", lax.rem(f + o, nf))

    def c_copy(t, o):
        return remote(rbuf.at[t, 0], rbuf.at[t, BLOCK[ns - o]], c_s.at[t, o - 1], c_r.at[t, o - 1], "samp", lax.rem(y + o, ns))

    def start_a(t, o):
        place = pl.ds((BLOCK[o] - 1) * rows, rows)
        usend[t, o] = ucol[place, :].T + urow[:, place]
        a_copy(t, o).start()

    def finish_a(t, total):
        for o in range(1, ns):
            a_copy(t, o).wait_recv()
        for o in range(1, ns):
            total = total + rsbuf[t, o]
        return total

    def sum_blocks(t, term):
        agbuf[t, f] = term.astype(jnp.bfloat16)
        for o in far_first(nf):
            b_copy(t, o, f).start()
        for o in range(1, nf):
            b_copy(t, o, lax.rem(f + nf - o, nf)).wait_recv()
        total = agbuf[t, 0].astype(jnp.float32)
        for j in range(1, nf):
            total = total + agbuf[t, j].astype(jnp.float32)
        return total

    def start_c(t):
        rbuf[t, 0] = rstate[...].astype(jnp.bfloat16)
        for o in far_first(ns):
            c_copy(t, o).start()

    def finish_c(t):
        for o in range(1, ns):
            c_copy(t, o).wait_recv()

    rstate[...] = yt_ref[...] - sum_blocks(0, first)
    start_c(0)

    def start_direct(k):
        for d in range(2):
            direct_copy(d, k).start()

    each(CHUNKS, start_direct)

    def start_forward(i):
        for d in range(2):
            relay_copy(d, i).wait_recv()
            forward_copy(d, i).start()

    each(half, start_forward)

    parts = chunk // sub

    def own_grad(k):
        for s in range(parts):
            part = pl.ds(s * sub, sub)
            gbuf[k, :, part] = jnp.dot(mine_low, xbuf[k, :rows, part], preferred_element_type=jnp.float32)

    def advance(k, s, resid):
        part = pl.ds(s * sub, sub)
        if resid.shape[1] == samples:
            grad = jnp.dot(resid, xbuf[k, :, part], preferred_element_type=jnp.float32) * inv
        else:
            grad = (gbuf[k, :, part] + jnp.dot(resid, xbuf[k, rows:, part], preferred_element_type=jnp.float32)) * inv
        place = pl.ds(pl.multiple_of(y * own + k * chunk + s * sub, sub), sub)
        w_part = wout[:, place]
        delta = ebuf[k, :, part] * (grad - ridge * w_part)
        wout[:, place] = w_part + COMBINE_WEIGHT * delta
        low = delta.astype(jnp.bfloat16)
        dbuf[k, :, part] = low
        return low

    def other_rows(first_row, k, low_of):
        col, row = None, None
        for s in range(parts):
            low = low_of(s)
            x_part = xbuf[k, first_row:, pl.ds(s * sub, sub)]
            if s < STREAM * parts:
                term = lax.dot_general(x_part, low, NT, preferred_element_type=jnp.float32)
                col = term if col is None else col + term
            else:
                term = lax.dot_general(low, x_part, NT, preferred_element_type=jnp.float32)
                row = term if row is None else row + term
        if col is not None:
            ucol[first_row - rows:, :] += col
        if row is not None:
            urow[:, first_row - rows:] += row

    def sweep_chunk(k, resid):
        other_rows(rows, k, lambda s: advance(k, s, resid))

    def own_rows(i, acc):
        for k in (2 * i, 2 * i + 1):
            for s in range(0, parts, 1):
                part = pl.ds(s * sub, 1 * sub)
                acc = acc + lax.dot_general(xbuf[k, :rows, part], dbuf[k, :, part], NT, preferred_element_type=jnp.float32)
        return acc

    def near_rows(i, carry):
        col, row = carry
        for k in (2 * i, 2 * i + 1):
            col = col + lax.dot_general(xbuf[k, 2 * rows:3 * rows, :], dbuf[k], NT, preferred_element_type=jnp.float32)
            row = row + lax.dot_general(dbuf[k], xbuf[k, 3 * rows:, :], NT, preferred_element_type=jnp.float32)
        return col, row

    def pair_rows(first_row, last_row, i):
        col, row = None, None
        held, out = pl.ds(first_row, last_row - first_row), pl.ds(first_row - rows, last_row - first_row)
        for s in range(0, parts, 1):
            part = pl.ds(s * sub, 1 * sub)
            term = lax.dot_general(xbuf[2 * i, held, part], dbuf[2 * i, :, part], NT, preferred_element_type=jnp.float32)
            col = term if col is None else col + term
            term = lax.dot_general(dbuf[2 * i + 1, :, part], xbuf[2 * i + 1, held, part], NT, preferred_element_type=jnp.float32)
            row = term if row is None else row + term
        ucol[out, :] += col
        urow[:, out] += row

    def arriving(i):
        for d in range(2):
            k = 2 * i + d
            own_copy(k).wait()
            w_load(k).wait()
            e_load(k).wait()
            for e in range(2):
                direct_copy(e, k).wait_recv()
            forward_copy(d, i).wait_recv()
            sweep_chunk(k, resid)

    def staying(i):
        for k in (2 * i, 2 * i + 1):
            for s in range(parts):
                advance(k, s, resid)

    def send_w(k):
        for d in range(2):
            wd_copy(d, k, y).start()

    def leaving(k):
        for s in range(parts):
            advance(k, s, resid)

        @pl.when(k > 0)
        def _():
            send_w(k - 1)

    for t in range(SWEEPS):
        ucol[...] = jnp.zeros_like(ucol)
        urow[...] = jnp.zeros_like(urow)
        if t:
            mine_low = rbuf[t, 0]
            each(CHUNKS, own_grad)
        finish_c(t)
        resid = jnp.concatenate([rbuf[t, b] for b in range(1 if t else 0, ns)], axis=1)
        if t == 0:
            each(half, arriving)
            start_a(t, 2)
        else:
            if t < SWEEPS - 1:
                each(half, staying)
            else:
                each(CHUNKS, leaving)
                send_w(CHUNKS - 1)
            each(half, functools.partial(pair_rows, rows, 2 * rows))
            start_a(t, 2)
            zeros = jnp.zeros((rows, targets), jnp.float32), jnp.zeros((targets, rows), jnp.float32)
            ucol[rows:2 * rows, :], urow[:, 2 * rows:] = lax.fori_loop(0, half, near_rows, zeros)
        start_a(t, 1)
        start_a(t, ns - 1)
        mine = lax.fori_loop(0, half, own_rows, jnp.zeros((rows, targets), jnp.float32)).T
        if t < SWEEPS - 1:
            rstate[...] = rstate[...] - COMBINE_WEIGHT * sum_blocks(t + 1, finish_a(t, mine))
            start_c(t + 1)

    def start_wf(i):
        for d in range(2):
            k = 2 * i + d
            for e in range(2):
                wd_copy(e, k, ring[1 - e]).wait_recv()
            wf_copy(d, i, ring[1 - d]).start()

    def start_wf_pair(i):
        start_wf(i)

    each(half, start_wf_pair)
    rout[...] = rstate[...] - COMBINE_WEIGHT * sum_blocks(SWEEPS, finish_a(SWEEPS - 1, mine))

    def finish_half(i):
        for d in range(2):
            relay_copy(d, i).wait_send()
            forward_copy(d, i).wait_send()
            wf_copy(d, i, far).wait_recv()
            wf_copy(d, i, ring[1 - d]).wait_send()

    def finish_full(k):
        for d in range(2):
            direct_copy(d, k).wait_send()
            wd_copy(d, k, y).wait_send()

    each(CHUNKS, finish_full)
    each(half, finish_half)
    for t in range(SWEEPS):
        for o in range(1, ns):
            a_copy(t, o).wait_send()
            c_copy(t, o).wait_send()
    for t in range(SWEEPS + 1):
        for o in range(1, nf):
            b_copy(t, o, f).wait_send()


def solution(mesh):
    ns, nf = mesh.shape["samp"], mesh.shape["feat"]

    def local_solve(x_loc, w_loc, y_loc, eta_loc):
        rows, feat_len = x_loc.shape
        targets = w_loc.shape[1]
        samples = rows * ns
        chunk = feat_len // ns // CHUNKS
        half = CHUNKS // 2
        dma = pltpu.SemaphoreType.DMA
        hbm = pl.BlockSpec(memory_space=pl.ANY)
        vmem = pl.BlockSpec(memory_space=pltpu.VMEM)
        small = feat_len * targets
        w_out, r_out, _ = pl.pallas_call(
            functools.partial(kernel, ns, nf),
            out_shape=(pltpu.VMEM((targets, feat_len), jnp.float32), pltpu.VMEM((targets, rows), jnp.float32),
                       jax.ShapeDtypeStruct((2, half, rows, chunk), jnp.bfloat16)),
            in_specs=[hbm, hbm, vmem, hbm],
            out_specs=(vmem, vmem, hbm),
            scratch_shapes=[
                pltpu.VMEM((CHUNKS, samples, chunk), jnp.bfloat16),
                pltpu.VMEM((CHUNKS, targets, chunk), jnp.float32),
                pltpu.VMEM((CHUNKS, targets, chunk), jnp.bfloat16),
                pltpu.VMEM((CHUNKS, 1, chunk), jnp.float32),
                pltpu.VMEM((V_SLOTS, rows, chunk), jnp.bfloat16),
                pltpu.VMEM((V_SLOTS, targets, chunk), jnp.float32),
                pltpu.VMEM((SWEEPS, ns, targets, rows), jnp.float32),
                pltpu.VMEM((SWEEPS, ns, targets, rows), jnp.float32),
                pltpu.VMEM((SWEEPS + 1, nf, targets, rows), jnp.bfloat16),
                pltpu.VMEM((SWEEPS, ns, targets, rows), jnp.bfloat16),
                pltpu.VMEM((targets, rows), jnp.float32),
                pltpu.VMEM((samples - rows, targets), jnp.float32),
                pltpu.VMEM((targets, samples - rows), jnp.float32),
                dma((CHUNKS,)), dma((CHUNKS,)), dma((CHUNKS,)), dma((2, V_SLOTS)),
                dma((2, half)), dma((2, half)), dma((2, CHUNKS)), dma((2, CHUNKS)), dma((2, half)), dma((2, half)),
                dma((SWEEPS, ns - 1)), dma((SWEEPS, ns - 1)),
                dma((SWEEPS + 1, nf - 1)), dma((SWEEPS + 1, nf - 1)),
                dma((SWEEPS, ns - 1)), dma((SWEEPS, ns - 1)),
                dma((2, CHUNKS)), dma((2, CHUNKS)), dma((2, half)), dma((2, half)),
            ],
            compiler_params=pltpu.CompilerParams(collective_id=0, has_side_effects=True, vmem_limit_bytes=47 * 1024 * 1024),
            cost_estimate=pl.CostEstimate(flops=2 * rows * small * (2 * SWEEPS + 1), bytes_accessed=8 * small + 4 * rows * feat_len,
                                          transcendentals=0),
            name="ridge_sweeps",
        )(x_loc, w_loc.T, y_loc.T, eta_loc.reshape(1, feat_len))
        pieces = 8

        def put(w_ref, r_ref, w_hbm, r_hbm, sem):
            width = feat_len // pieces
            copies = [pltpu.make_async_copy(w_ref.at[:, pl.ds(i * width, width)], w_hbm.at[:, pl.ds(i * width, width)], sem.at[i])
                      for i in range(pieces)]
            copies.append(pltpu.make_async_copy(r_ref, r_hbm, sem.at[pieces]))
            for copy in copies:
                copy.start()
            for copy in copies:
                copy.wait()

        w_out, r_out = pl.pallas_call(
            put,
            out_shape=(jax.ShapeDtypeStruct((targets, feat_len), jnp.float32), jax.ShapeDtypeStruct((targets, rows), jnp.float32)),
            in_specs=[vmem, vmem],
            out_specs=(hbm, hbm),
            scratch_shapes=[dma((pieces + 1,))],
            compiler_params=pltpu.CompilerParams(vmem_limit_bytes=1024 * 1024),
            name="put_results",
        )(pltpu.with_memory_space_constraint(w_out, pltpu.VMEM), pltpu.with_memory_space_constraint(r_out, pltpu.VMEM))
        return w_out.T, r_out.T

    return jax.shard_map(
        local_solve,
        mesh=mesh,
        in_specs=(P(("prob", "samp"), "feat"), P(("prob", "feat"), None), P(("prob", "samp"), None), P(("prob", "feat"))),
        out_specs=(P(("prob", "feat"), None), P(("prob", "samp"), None)),
        check_vma=False,
    )
```

```python
import functools

import jax
import jax.numpy as jnp
from jax import lax
from jax.experimental import pallas as pl
from jax.experimental.pallas import tpu as pltpu
from jax.sharding import PartitionSpec as P

SWEEPS = 4
COMBINE_WEIGHT = 0.8
RIDGE_SCALE = 0.1
CHUNKS = 16
SUB = 512
STREAM = 0.5
EARLY = 4
V_SLOTS = 3
MESH = pl.DeviceIdType.MESH
NT = (((1,), (1,)), ((), ()))


BLOCK = (0, 2, 1, 3)


def far_first(count):
    return sorted(range(1, count), key=lambda o: -min(o, count - o))


def kernel(ns, nf, x_hbm, wt_hbm, yt_ref, eta_hbm, wout, rout, relay, xbuf, gbuf, dbuf, ebuf, vx, vw, usend, rsbuf, agbuf, rbuf, rstate, ucol, urow,
           own_sem, w_sem, e_sem, v_sem, rel_s, rel_r, dir_s, dir_r, fwd_s, fwd_r, a_s, a_r, b_s, b_r, c_s, c_r,
           wd_s, wd_r, wf_s, wf_r):
    y, f = lax.axis_index("samp"), lax.axis_index("feat")
    rows, feat_len = x_hbm.shape
    targets = wt_hbm.shape[0]
    own = feat_len // ns
    chunk = own // CHUNKS
    half = CHUNKS // 2
    sub = min(SUB, chunk)
    samples = rows * ns
    inv = 1.0 / samples
    ridge = RIDGE_SCALE * (feat_len * nf) / samples
    up, down, far = lax.rem(y + 1, ns), lax.rem(y + ns - 1, ns), lax.rem(y + 2, ns)
    ring = (up, down)

    def cols(owner, k):
        return pl.ds(pl.multiple_of(owner * own + k * chunk, chunk), chunk)

    def rows_of(o):
        return pl.ds(BLOCK[o] * rows, rows)

    def remote(src, dst, send, recv, axis, dev):
        return pltpu.make_async_remote_copy(src_ref=src, dst_ref=dst, send_sem=send, recv_sem=recv,
                                            device_id={axis: dev}, device_id_type=MESH)

    def own_copy(k):
        return pltpu.make_async_copy(x_hbm.at[:, cols(y, k)], xbuf.at[k, rows_of(0), :], own_sem.at[k])

    def w_load(k):
        return pltpu.make_async_copy(wt_hbm.at[:, cols(y, k)], wout.at[:, cols(y, k)], w_sem.at[k])

    def e_load(k):
        return pltpu.make_async_copy(eta_hbm.at[:, cols(y, k)], ebuf.at[k], e_sem.at[k])

    v_steps = ns * CHUNKS

    def v_cols(k):
        return pl.ds(pl.multiple_of(k * chunk, chunk), chunk)

    def v_load(k, slot):
        return (pltpu.make_async_copy(x_hbm.at[:, v_cols(k)], vx.at[slot], v_sem.at[0, slot]),
                pltpu.make_async_copy(wt_hbm.at[:, v_cols(k)], vw.at[slot], v_sem.at[1, slot]))

    def relay_copy(d, i):
        return remote(x_hbm.at[:, cols(far, 2 * i + d)], relay.at[d, i], rel_s.at[d, i], rel_r.at[d, i], "samp", ring[d])

    def direct_copy(d, k):
        return remote(x_hbm.at[:, cols(ring[d], k)], xbuf.at[k, rows_of((ns - 1, 1)[d]), :], dir_s.at[d, k], dir_r.at[d, k], "samp", ring[d])

    def forward_copy(d, i):
        return remote(relay.at[d, i], xbuf.at[2 * i + d, rows_of(2), :], fwd_s.at[d, i], fwd_r.at[d, i], "samp", ring[d])

    def wd_copy(d, k, owner):
        return remote(wout.at[:, cols(y, k)], wout.at[:, cols(owner, k)], wd_s.at[d, k], wd_r.at[d, k], "samp", ring[d])

    def wf_copy(d, i, owner):
        part = wout.at[:, cols(owner, 2 * i + d)]
        return remote(part, part, wf_s.at[d, i], wf_r.at[d, i], "samp", ring[d])

    def each(count, body, start=0):
        lax.fori_loop(start, count, lambda i, c: (body(i), c)[1], 0)

    def start_local(k):
        own_copy(k).start()
        w_load(k).start()
        e_load(k).start()

    barrier = pltpu.get_barrier_semaphore()
    for o in range(1, ns):
        pl.semaphore_signal(barrier, inc=1, device_id={"samp": lax.rem(y + o, ns)}, device_id_type=MESH)
    for o in range(1, nf):
        pl.semaphore_signal(barrier, inc=1, device_id={"feat": lax.rem(f + o, nf)}, device_id_type=MESH)
    for k in range(V_SLOTS):
        for copy in v_load(k, k):
            copy.start()
    pl.semaphore_wait(barrier, ns - 1 + nf - 1)

    def start_relay(i):
        for d in range(2):
            relay_copy(d, i).start()

    each(half, start_relay)

    def v_step(k, acc):
        slot = lax.rem(k, V_SLOTS)
        for copy in v_load(k, slot):
            copy.wait()
        low = vw[slot].astype(jnp.bfloat16)
        acc = acc + lax.dot_general(low, vx[slot], NT, preferred_element_type=jnp.float32)

        @pl.when(k + V_SLOTS < v_steps)
        def _():
            for copy in v_load(k + V_SLOTS, slot):
                copy.start()

        return acc

    first = lax.fori_loop(0, v_steps, v_step, jnp.zeros((targets, rows), jnp.float32))
    each(CHUNKS, start_local)

    def a_copy(t, o):
        return remote(usend.at[t, o], rsbuf.at[t, ns - o], a_s.at[t, o - 1], a_r.at[t, o - 1], "samp", lax.rem(y + o, ns))

    def b_copy(t, o, place):
        return remote(agbuf.at[t, f], agbuf.at[t, place], b_s.at[t, o - 1], b_r.at[t, o - 1], "feat", lax.rem(f + o, nf))

    def c_copy(t, o):
        return remote(rbuf.at[t, 0], rbuf.at[t, BLOCK[ns - o]], c_s.at[t, o - 1], c_r.at[t, o - 1], "samp", lax.rem(y + o, ns))

    def start_a(t, o):
        place = pl.ds((BLOCK[o] - 1) * rows, rows)
        usend[t, o] = ucol[place, :].T + urow[:, place]
        a_copy(t, o).start()

    def finish_a(t, total):
        for o in range(1, ns):
            a_copy(t, o).wait_recv()
        for o in range(1, ns):
            total = total + rsbuf[t, o]
        return total

    def sum_blocks(t, term):
        agbuf[t, f] = term.astype(jnp.bfloat16)
        for o in far_first(nf):
            b_copy(t, o, f).start()
        for o in range(1, nf):
            b_copy(t, o, lax.rem(f + nf - o, nf)).wait_recv()
        total = agbuf[t, 0].astype(jnp.float32)
        for j in range(1, nf):
            total = total + agbuf[t, j].astype(jnp.float32)
        return total

    def start_c(t):
        rbuf[t, 0] = rstate[...].astype(jnp.bfloat16)
        for o in far_first(ns):
            c_copy(t, o).start()

    def finish_c(t, offsets):
        for o in offsets:
            c_copy(t, o).wait_recv()
        return jnp.concatenate([rbuf[t, b] for b in sorted(BLOCK[o] for o in offsets)], axis=1)

    rstate[...] = yt_ref[...] - sum_blocks(0, first)
    start_c(0)

    def start_direct(k):
        for d in range(2):
            direct_copy(d, k).start()

    each(CHUNKS, start_direct)

    def start_forward(i):
        for d in range(2):
            relay_copy(d, i).wait_recv()
            forward_copy(d, i).start()

    each(half, start_forward)

    parts = chunk // sub

    def rows_grad(low, first_row, k, part):
        held = pl.ds(first_row, low.shape[1])
        return jnp.dot(low, xbuf[k, held, part], preferred_element_type=jnp.float32)

    def own_grad(low, k):
        for s in range(parts):
            part = pl.ds(s * sub, sub)
            gbuf[k, :, part] = rows_grad(low, 0, k, part)

    def near_grad(low, k):
        for s in range(parts):
            part = pl.ds(s * sub, sub)
            gbuf[k, :, part] += rows_grad(low, 2 * rows, k, part)

    def ready_grad(own_low, near_low, k):
        own_copy(k).wait()
        for e in range(2):
            direct_copy(e, k).wait_recv()
        for s in range(parts):
            part = pl.ds(s * sub, sub)
            gbuf[k, :, part] = rows_grad(own_low, 0, k, part) + rows_grad(near_low, 2 * rows, k, part)

    def advance(k, s, low):
        part = pl.ds(s * sub, sub)
        grad = (gbuf[k, :, part] + rows_grad(low, rows, k, part)) * inv
        place = pl.ds(pl.multiple_of(y * own + k * chunk + s * sub, sub), sub)
        w_part = wout[:, place]
        delta = ebuf[k, :, part] * (grad - ridge * w_part)
        wout[:, place] = w_part + COMBINE_WEIGHT * delta
        low = delta.astype(jnp.bfloat16)
        dbuf[k, :, part] = low
        return low

    def other_rows(first_row, k, low_of):
        col, row = None, None
        for s in range(parts):
            low = low_of(s)
            x_part = xbuf[k, first_row:, pl.ds(s * sub, sub)]
            if s < STREAM * parts:
                term = lax.dot_general(x_part, low, NT, preferred_element_type=jnp.float32)
                col = term if col is None else col + term
            else:
                term = lax.dot_general(low, x_part, NT, preferred_element_type=jnp.float32)
                row = term if row is None else row + term
        if col is not None:
            ucol[first_row - rows:, :] += col
        if row is not None:
            urow[:, first_row - rows:] += row


    def own_rows(i, acc):
        for k in (2 * i, 2 * i + 1):
            for s in range(0, parts, 1):
                part = pl.ds(s * sub, 1 * sub)
                acc = acc + lax.dot_general(xbuf[k, :rows, part], dbuf[k, :, part], NT, preferred_element_type=jnp.float32)
        return acc

    def near_rows(i, carry):
        col, row = carry
        for k in (2 * i, 2 * i + 1):
            col = col + lax.dot_general(xbuf[k, 2 * rows:3 * rows, :], dbuf[k], NT, preferred_element_type=jnp.float32)
            row = row + lax.dot_general(dbuf[k], xbuf[k, 3 * rows:, :], NT, preferred_element_type=jnp.float32)
        return col, row

    def pair_rows(first_row, last_row, i):
        col, row = None, None
        held, out = pl.ds(first_row, last_row - first_row), pl.ds(first_row - rows, last_row - first_row)
        for s in range(0, parts, 1):
            part = pl.ds(s * sub, 1 * sub)
            term = lax.dot_general(xbuf[2 * i, held, part], dbuf[2 * i, :, part], NT, preferred_element_type=jnp.float32)
            col = term if col is None else col + term
            term = lax.dot_general(dbuf[2 * i + 1, :, part], xbuf[2 * i + 1, held, part], NT, preferred_element_type=jnp.float32)
            row = term if row is None else row + term
        ucol[out, :] += col
        urow[:, out] += row

    def arriving(low, i):
        for d in range(2):
            k = 2 * i + d
            w_load(k).wait()
            e_load(k).wait()
            forward_copy(d, i).wait_recv()
            other_rows(rows, k, lambda s: advance(k, s, low))

    def staying(low, i):
        for k in (2 * i, 2 * i + 1):
            for s in range(parts):
                advance(k, s, low)

    def send_w(k):
        for d in range(2):
            wd_copy(d, k, y).start()

    def leaving(low, k):
        for s in range(parts):
            advance(k, s, low)

        @pl.when(k > 0)
        def _():
            send_w(k - 1)

    for t in range(SWEEPS):
        ucol[...] = jnp.zeros_like(ucol)
        urow[...] = jnp.zeros_like(urow)
        if t == 0:
            near = finish_c(t, (1, ns - 1))
            each(CHUNKS, functools.partial(ready_grad, rbuf[t, 0], near))
            each(half, functools.partial(arriving, finish_c(t, (2,))))
            start_a(t, 2)
        else:
            each(CHUNKS, functools.partial(own_grad, rbuf[t, 0]))
            near = finish_c(t, (1, ns - 1))
            each(EARLY, functools.partial(near_grad, near))
            far_low = finish_c(t, (2,))
            other_low = jnp.concatenate([far_low, near], axis=1)
            if t < SWEEPS - 1:
                each(EARLY // 2, functools.partial(staying, far_low))
                each(half, functools.partial(staying, other_low), EARLY // 2)
            else:
                each(EARLY, functools.partial(leaving, far_low))
                each(CHUNKS, functools.partial(leaving, other_low), EARLY)
                send_w(CHUNKS - 1)
            each(half, functools.partial(pair_rows, rows, 2 * rows))
            start_a(t, 2)
            zeros = jnp.zeros((rows, targets), jnp.float32), jnp.zeros((targets, rows), jnp.float32)
            ucol[rows:2 * rows, :], urow[:, 2 * rows:] = lax.fori_loop(0, half, near_rows, zeros)
        start_a(t, 1)
        start_a(t, ns - 1)
        mine = lax.fori_loop(0, half, own_rows, jnp.zeros((rows, targets), jnp.float32)).T
        if t < SWEEPS - 1:
            rstate[...] = rstate[...] - COMBINE_WEIGHT * sum_blocks(t + 1, finish_a(t, mine))
            start_c(t + 1)

    def start_wf(i):
        for d in range(2):
            k = 2 * i + d
            for e in range(2):
                wd_copy(e, k, ring[1 - e]).wait_recv()
            wf_copy(d, i, ring[1 - d]).start()

    def start_wf_pair(i):
        start_wf(i)

    each(half, start_wf_pair)
    rout[...] = rstate[...] - COMBINE_WEIGHT * sum_blocks(SWEEPS, finish_a(SWEEPS - 1, mine))

    def finish_full(k):
        for d in range(2):
            direct_copy(d, k).wait_send()
            wd_copy(d, k, y).wait_send()

    def finish_half(i):
        for d in range(2):
            relay_copy(d, i).wait_send()
            forward_copy(d, i).wait_send()

    def finish_last(i):
        for d in range(2):
            wf_copy(d, i, ring[1 - d]).wait_send()
            wf_copy(d, i, far).wait_recv()

    each(CHUNKS, finish_full)
    each(half, finish_half)
    for t in range(SWEEPS):
        for o in range(1, ns):
            a_copy(t, o).wait_send()
            c_copy(t, o).wait_send()
    for t in range(SWEEPS + 1):
        for o in range(1, nf):
            b_copy(t, o, f).wait_send()
    each(half, finish_last)


def solution(mesh):
    ns, nf = mesh.shape["samp"], mesh.shape["feat"]

    def local_solve(x_loc, w_loc, y_loc, eta_loc):
        rows, feat_len = x_loc.shape
        targets = w_loc.shape[1]
        samples = rows * ns
        chunk = feat_len // ns // CHUNKS
        half = CHUNKS // 2
        dma = pltpu.SemaphoreType.DMA
        hbm = pl.BlockSpec(memory_space=pl.ANY)
        vmem = pl.BlockSpec(memory_space=pltpu.VMEM)
        small = feat_len * targets
        w_out, r_out, _ = pl.pallas_call(
            functools.partial(kernel, ns, nf),
            out_shape=(pltpu.VMEM((targets, feat_len), jnp.float32), pltpu.VMEM((targets, rows), jnp.float32),
                       jax.ShapeDtypeStruct((2, half, rows, chunk), jnp.bfloat16)),
            in_specs=[hbm, hbm, vmem, hbm],
            out_specs=(vmem, vmem, hbm),
            scratch_shapes=[
                pltpu.VMEM((CHUNKS, samples, chunk), jnp.bfloat16),
                pltpu.VMEM((CHUNKS, targets, chunk), jnp.float32),
                pltpu.VMEM((CHUNKS, targets, chunk), jnp.bfloat16),
                pltpu.VMEM((CHUNKS, 1, chunk), jnp.float32),
                pltpu.VMEM((V_SLOTS, rows, chunk), jnp.bfloat16),
                pltpu.VMEM((V_SLOTS, targets, chunk), jnp.float32),
                pltpu.VMEM((SWEEPS, ns, targets, rows), jnp.float32),
                pltpu.VMEM((SWEEPS, ns, targets, rows), jnp.float32),
                pltpu.VMEM((SWEEPS + 1, nf, targets, rows), jnp.bfloat16),
                pltpu.VMEM((SWEEPS, ns, targets, rows), jnp.bfloat16),
                pltpu.VMEM((targets, rows), jnp.float32),
                pltpu.VMEM((samples - rows, targets), jnp.float32),
                pltpu.VMEM((targets, samples - rows), jnp.float32),
                dma((CHUNKS,)), dma((CHUNKS,)), dma((CHUNKS,)), dma((2, V_SLOTS)),
                dma((2, half)), dma((2, half)), dma((2, CHUNKS)), dma((2, CHUNKS)), dma((2, half)), dma((2, half)),
                dma((SWEEPS, ns - 1)), dma((SWEEPS, ns - 1)),
                dma((SWEEPS + 1, nf - 1)), dma((SWEEPS + 1, nf - 1)),
                dma((SWEEPS, ns - 1)), dma((SWEEPS, ns - 1)),
                dma((2, CHUNKS)), dma((2, CHUNKS)), dma((2, half)), dma((2, half)),
            ],
            compiler_params=pltpu.CompilerParams(collective_id=0, has_side_effects=True, vmem_limit_bytes=47 * 1024 * 1024),
            cost_estimate=pl.CostEstimate(flops=2 * rows * small * (2 * SWEEPS + 1), bytes_accessed=8 * small + 4 * rows * feat_len,
                                          transcendentals=0),
            name="ridge_sweeps",
        )(x_loc, w_loc.T, y_loc.T, eta_loc.reshape(1, feat_len))
        pieces = targets // 8

        def put(w_ref, r_ref, w_hbm, r_hbm, sem):
            width = targets // pieces
            copies = [pltpu.make_async_copy(w_ref.at[pl.ds(i * width, width), :], w_hbm.at[pl.ds(i * width, width), :], sem.at[i])
                      for i in range(pieces)]
            copies.append(pltpu.make_async_copy(r_ref, r_hbm, sem.at[pieces]))
            for copy in copies:
                copy.start()
            for copy in copies:
                copy.wait()

        w_out, r_out = pl.pallas_call(
            put,
            out_shape=(jax.ShapeDtypeStruct((targets, feat_len), jnp.float32), jax.ShapeDtypeStruct((targets, rows), jnp.float32)),
            in_specs=[vmem, vmem],
            out_specs=(hbm, hbm),
            scratch_shapes=[dma((pieces + 1,))],
            compiler_params=pltpu.CompilerParams(vmem_limit_bytes=1024 * 1024),
            name="put_results",
        )(pltpu.with_memory_space_constraint(w_out, pltpu.VMEM), pltpu.with_memory_space_constraint(r_out, pltpu.VMEM))
        return w_out.T, r_out.T

    return jax.shard_map(
        local_solve,
        mesh=mesh,
        in_specs=(P(("prob", "samp"), "feat"), P(("prob", "feat"), None), P(("prob", "samp"), None), P(("prob", "feat"))),
        out_specs=(P(("prob", "feat"), None), P(("prob", "samp"), None)),
        check_vma=False,
    )
```

```python
import functools

import jax
import jax.numpy as jnp
from jax import lax
from jax.experimental import pallas as pl
from jax.experimental.pallas import tpu as pltpu
from jax.sharding import PartitionSpec as P

SWEEPS = 4
COMBINE_WEIGHT = 0.8
RIDGE_SCALE = 0.1
CHUNKS = 16
SUB = 512
STREAM = 0.5
V_SLOTS = 3
MESH = pl.DeviceIdType.MESH
NT = (((1,), (1,)), ((), ()))


BLOCK = (0, 2, 1, 3)


def far_first(count):
    return sorted(range(1, count), key=lambda o: -min(o, count - o))


def kernel(ns, nf, x_hbm, wt_hbm, yt_ref, eta_hbm, wout, rout, relay, xbuf, gbuf, dbuf, ebuf, vx, vw, usend, rsbuf, agbuf, rbuf, rstate, ucol, urow,
           own_sem, w_sem, e_sem, v_sem, rel_s, rel_r, dir_s, dir_r, fwd_s, fwd_r, a_s, a_r, b_s, b_r, c_s, c_r,
           wd_s, wd_r, wf_s, wf_r):
    y, f = lax.axis_index("samp"), lax.axis_index("feat")
    rows, feat_len = x_hbm.shape
    targets = wt_hbm.shape[0]
    own = feat_len // ns
    chunk = own // CHUNKS
    half = CHUNKS // 2
    sub = min(SUB, chunk)
    samples = rows * ns
    inv = 1.0 / samples
    ridge = RIDGE_SCALE * (feat_len * nf) / samples
    up, down, far = lax.rem(y + 1, ns), lax.rem(y + ns - 1, ns), lax.rem(y + 2, ns)
    ring = (up, down)

    def cols(owner, k):
        return pl.ds(pl.multiple_of(owner * own + k * chunk, chunk), chunk)

    def rows_of(o):
        return pl.ds(BLOCK[o] * rows, rows)

    def remote(src, dst, send, recv, axis, dev):
        return pltpu.make_async_remote_copy(src_ref=src, dst_ref=dst, send_sem=send, recv_sem=recv,
                                            device_id={axis: dev}, device_id_type=MESH)

    def own_copy(k):
        return pltpu.make_async_copy(x_hbm.at[:, cols(y, k)], xbuf.at[k, rows_of(0), :], own_sem.at[k])

    def w_load(k):
        return pltpu.make_async_copy(wt_hbm.at[:, cols(y, k)], wout.at[:, cols(y, k)], w_sem.at[k])

    def e_load(k):
        return pltpu.make_async_copy(eta_hbm.at[:, cols(y, k)], ebuf.at[k], e_sem.at[k])

    v_steps = ns * CHUNKS

    def v_cols(k):
        return pl.ds(pl.multiple_of(k * chunk, chunk), chunk)

    def v_load(k, slot):
        return (pltpu.make_async_copy(x_hbm.at[:, v_cols(k)], vx.at[slot], v_sem.at[0, slot]),
                pltpu.make_async_copy(wt_hbm.at[:, v_cols(k)], vw.at[slot], v_sem.at[1, slot]))

    def relay_copy(d, i):
        return remote(x_hbm.at[:, cols(far, 2 * i + d)], relay.at[d, i], rel_s.at[d, i], rel_r.at[d, i], "samp", ring[d])

    def direct_copy(d, k):
        return remote(x_hbm.at[:, cols(ring[d], k)], xbuf.at[k, rows_of((ns - 1, 1)[d]), :], dir_s.at[d, k], dir_r.at[d, k], "samp", ring[d])

    def forward_copy(d, i):
        return remote(relay.at[d, i], xbuf.at[2 * i + d, rows_of(2), :], fwd_s.at[d, i], fwd_r.at[d, i], "samp", ring[d])

    def wd_copy(d, k, owner):
        return remote(wout.at[:, cols(y, k)], wout.at[:, cols(owner, k)], wd_s.at[d, k], wd_r.at[d, k], "samp", ring[d])

    def wf_copy(d, i, owner):
        part = wout.at[:, cols(owner, 2 * i + d)]
        return remote(part, part, wf_s.at[d, i], wf_r.at[d, i], "samp", ring[d])

    def each(count, body):
        lax.fori_loop(0, count, lambda i, c: (body(i), c)[1], 0)

    def start_local(k):
        own_copy(k).start()
        w_load(k).start()
        e_load(k).start()

    barrier = pltpu.get_barrier_semaphore()
    for o in range(1, ns):
        pl.semaphore_signal(barrier, inc=1, device_id={"samp": lax.rem(y + o, ns)}, device_id_type=MESH)
    for o in range(1, nf):
        pl.semaphore_signal(barrier, inc=1, device_id={"feat": lax.rem(f + o, nf)}, device_id_type=MESH)
    for k in range(V_SLOTS):
        for copy in v_load(k, k):
            copy.start()
    pl.semaphore_wait(barrier, ns - 1 + nf - 1)

    def start_relay(i):
        for d in range(2):
            relay_copy(d, i).start()

    each(half, start_relay)

    def v_step(k, acc):
        slot = lax.rem(k, V_SLOTS)
        for copy in v_load(k, slot):
            copy.wait()
        low = vw[slot].astype(jnp.bfloat16)
        acc = acc + lax.dot_general(low, vx[slot], NT, preferred_element_type=jnp.float32)

        @pl.when(k + V_SLOTS < v_steps)
        def _():
            for copy in v_load(k + V_SLOTS, slot):
                copy.start()

        return acc

    first = lax.fori_loop(0, v_steps, v_step, jnp.zeros((targets, rows), jnp.float32))
    each(CHUNKS, start_local)

    def a_copy(t, o):
        return remote(usend.at[t, o], rsbuf.at[t, ns - o], a_s.at[t, o - 1], a_r.at[t, o - 1], "samp", lax.rem(y + o, ns))

    def b_copy(t, o, place):
        return remote(agbuf.at[t, f], agbuf.at[t, place], b_s.at[t, o - 1], b_r.at[t, o - 1], "feat", lax.rem(f + o, nf))

    def c_copy(t, o):
        return remote(rbuf.at[t, 0], rbuf.at[t, BLOCK[ns - o]], c_s.at[t, o - 1], c_r.at[t, o - 1], "samp", lax.rem(y + o, ns))

    def start_a(t, o):
        place = pl.ds((BLOCK[o] - 1) * rows, rows)
        usend[t, o] = ucol[place, :].T + urow[:, place]
        a_copy(t, o).start()

    def finish_a(t, total):
        for o in range(1, ns):
            a_copy(t, o).wait_recv()
        for o in range(1, ns):
            total = total + rsbuf[t, o]
        return total

    def sum_blocks(t, term):
        agbuf[t, f] = term.astype(jnp.bfloat16)
        for o in far_first(nf):
            b_copy(t, o, f).start()
        for o in range(1, nf):
            b_copy(t, o, lax.rem(f + nf - o, nf)).wait_recv()
        total = agbuf[t, 0].astype(jnp.float32)
        for j in range(1, nf):
            total = total + agbuf[t, j].astype(jnp.float32)
        return total

    def start_c(t):
        rbuf[t, 0] = rstate[...].astype(jnp.bfloat16)
        for o in far_first(ns):
            c_copy(t, o).start()

    def finish_c(t, offsets):
        for o in offsets:
            c_copy(t, o).wait_recv()
        return jnp.concatenate([rbuf[t, b] for b in sorted(BLOCK[o] for o in offsets)], axis=1)

    rstate[...] = yt_ref[...] - sum_blocks(0, first)
    start_c(0)

    def start_direct(k):
        for d in range(2):
            direct_copy(d, k).start()

    each(CHUNKS, start_direct)

    def start_forward(i):
        for d in range(2):
            relay_copy(d, i).wait_recv()
            forward_copy(d, i).start()

    each(half, start_forward)

    parts = chunk // sub

    def rows_grad(low, first_row, k, part):
        held = pl.ds(first_row, low.shape[1])
        return jnp.dot(low, xbuf[k, held, part], preferred_element_type=jnp.float32)

    def own_grad(low, k):
        for s in range(parts):
            part = pl.ds(s * sub, sub)
            gbuf[k, :, part] = rows_grad(low, 0, k, part)

    def ready_grad(own_low, near_low, k):
        own_copy(k).wait()
        for e in range(2):
            direct_copy(e, k).wait_recv()
        for s in range(parts):
            part = pl.ds(s * sub, sub)
            gbuf[k, :, part] = rows_grad(own_low, 0, k, part) + rows_grad(near_low, 2 * rows, k, part)

    def advance(k, s, low):
        part = pl.ds(s * sub, sub)
        grad = (gbuf[k, :, part] + rows_grad(low, rows, k, part)) * inv
        place = pl.ds(pl.multiple_of(y * own + k * chunk + s * sub, sub), sub)
        w_part = wout[:, place]
        delta = ebuf[k, :, part] * (grad - ridge * w_part)
        wout[:, place] = w_part + COMBINE_WEIGHT * delta
        low = delta.astype(jnp.bfloat16)
        dbuf[k, :, part] = low
        return low

    def other_rows(first_row, k, low_of):
        col, row = None, None
        for s in range(parts):
            low = low_of(s)
            x_part = xbuf[k, first_row:, pl.ds(s * sub, sub)]
            if s < STREAM * parts:
                term = lax.dot_general(x_part, low, NT, preferred_element_type=jnp.float32)
                col = term if col is None else col + term
            else:
                term = lax.dot_general(low, x_part, NT, preferred_element_type=jnp.float32)
                row = term if row is None else row + term
        if col is not None:
            ucol[first_row - rows:, :] += col
        if row is not None:
            urow[:, first_row - rows:] += row


    def own_rows(i, acc):
        for k in (2 * i, 2 * i + 1):
            for s in range(0, parts, 1):
                part = pl.ds(s * sub, 1 * sub)
                acc = acc + lax.dot_general(xbuf[k, :rows, part], dbuf[k, :, part], NT, preferred_element_type=jnp.float32)
        return acc

    def near_rows(i, carry):
        col, row = carry
        for k in (2 * i, 2 * i + 1):
            col = col + lax.dot_general(xbuf[k, 2 * rows:3 * rows, :], dbuf[k], NT, preferred_element_type=jnp.float32)
            row = row + lax.dot_general(dbuf[k], xbuf[k, 3 * rows:, :], NT, preferred_element_type=jnp.float32)
        return col, row

    def pair_rows(first_row, last_row, i):
        col, row = None, None
        held, out = pl.ds(first_row, last_row - first_row), pl.ds(first_row - rows, last_row - first_row)
        for s in range(0, parts, 1):
            part = pl.ds(s * sub, 1 * sub)
            term = lax.dot_general(xbuf[2 * i, held, part], dbuf[2 * i, :, part], NT, preferred_element_type=jnp.float32)
            col = term if col is None else col + term
            term = lax.dot_general(dbuf[2 * i + 1, :, part], xbuf[2 * i + 1, held, part], NT, preferred_element_type=jnp.float32)
            row = term if row is None else row + term
        ucol[out, :] += col
        urow[:, out] += row

    def arriving(low, i):
        for d in range(2):
            k = 2 * i + d
            w_load(k).wait()
            e_load(k).wait()
            forward_copy(d, i).wait_recv()
            other_rows(rows, k, lambda s: advance(k, s, low))

    def staying(low, i):
        for k in (2 * i, 2 * i + 1):
            for s in range(parts):
                advance(k, s, low)

    def send_w(k):
        for d in range(2):
            wd_copy(d, k, y).start()

    def leaving(low, k):
        for s in range(parts):
            advance(k, s, low)

        @pl.when(k > 0)
        def _():
            send_w(k - 1)

    for t in range(SWEEPS):
        ucol[...] = jnp.zeros_like(ucol)
        urow[...] = jnp.zeros_like(urow)
        if t == 0:
            near = finish_c(t, (1, ns - 1))
            each(CHUNKS, functools.partial(ready_grad, rbuf[t, 0], near))
            each(half, functools.partial(arriving, finish_c(t, (2,))))
            start_a(t, 2)
        else:
            each(CHUNKS, functools.partial(own_grad, rbuf[t, 0]))
            other_low = finish_c(t, (1, 2, ns - 1))
            if t < SWEEPS - 1:
                each(half, functools.partial(staying, other_low))
            else:
                each(CHUNKS, functools.partial(leaving, other_low))
                send_w(CHUNKS - 1)
            each(half, functools.partial(pair_rows, rows, 2 * rows))
            start_a(t, 2)
            zeros = jnp.zeros((rows, targets), jnp.float32), jnp.zeros((targets, rows), jnp.float32)
            ucol[rows:2 * rows, :], urow[:, 2 * rows:] = lax.fori_loop(0, half, near_rows, zeros)
        start_a(t, 1)
        start_a(t, ns - 1)
        mine = lax.fori_loop(0, half, own_rows, jnp.zeros((rows, targets), jnp.float32)).T
        if t < SWEEPS - 1:
            rstate[...] = rstate[...] - COMBINE_WEIGHT * sum_blocks(t + 1, finish_a(t, mine))
            start_c(t + 1)

    def start_wf(i):
        for d in range(2):
            k = 2 * i + d
            for e in range(2):
                wd_copy(e, k, ring[1 - e]).wait_recv()
            wf_copy(d, i, ring[1 - d]).start()

    def start_wf_pair(i):
        start_wf(i)

    each(half, start_wf_pair)
    rout[...] = rstate[...] - COMBINE_WEIGHT * sum_blocks(SWEEPS, finish_a(SWEEPS - 1, mine))

    def finish_full(k):
        for d in range(2):
            direct_copy(d, k).wait_send()
            wd_copy(d, k, y).wait_send()

    def finish_half(i):
        for d in range(2):
            relay_copy(d, i).wait_send()
            forward_copy(d, i).wait_send()

    def finish_last(i):
        for d in range(2):
            wf_copy(d, i, ring[1 - d]).wait_send()
            wf_copy(d, i, far).wait_recv()

    each(CHUNKS, finish_full)
    each(half, finish_half)
    for t in range(SWEEPS):
        for o in range(1, ns):
            a_copy(t, o).wait_send()
            c_copy(t, o).wait_send()
    for t in range(SWEEPS + 1):
        for o in range(1, nf):
            b_copy(t, o, f).wait_send()
    each(half, finish_last)


def solution(mesh):
    ns, nf = mesh.shape["samp"], mesh.shape["feat"]

    def local_solve(x_loc, w_loc, y_loc, eta_loc):
        rows, feat_len = x_loc.shape
        targets = w_loc.shape[1]
        samples = rows * ns
        chunk = feat_len // ns // CHUNKS
        half = CHUNKS // 2
        dma = pltpu.SemaphoreType.DMA
        hbm = pl.BlockSpec(memory_space=pl.ANY)
        vmem = pl.BlockSpec(memory_space=pltpu.VMEM)
        small = feat_len * targets
        w_out, r_out, _ = pl.pallas_call(
            functools.partial(kernel, ns, nf),
            out_shape=(pltpu.VMEM((targets, feat_len), jnp.float32), pltpu.VMEM((targets, rows), jnp.float32),
                       jax.ShapeDtypeStruct((2, half, rows, chunk), jnp.bfloat16)),
            in_specs=[hbm, hbm, vmem, hbm],
            out_specs=(vmem, vmem, hbm),
            scratch_shapes=[
                pltpu.VMEM((CHUNKS, samples, chunk), jnp.bfloat16),
                pltpu.VMEM((CHUNKS, targets, chunk), jnp.float32),
                pltpu.VMEM((CHUNKS, targets, chunk), jnp.bfloat16),
                pltpu.VMEM((CHUNKS, 1, chunk), jnp.float32),
                pltpu.VMEM((V_SLOTS, rows, chunk), jnp.bfloat16),
                pltpu.VMEM((V_SLOTS, targets, chunk), jnp.float32),
                pltpu.VMEM((SWEEPS, ns, targets, rows), jnp.float32),
                pltpu.VMEM((SWEEPS, ns, targets, rows), jnp.float32),
                pltpu.VMEM((SWEEPS + 1, nf, targets, rows), jnp.bfloat16),
                pltpu.VMEM((SWEEPS, ns, targets, rows), jnp.bfloat16),
                pltpu.VMEM((targets, rows), jnp.float32),
                pltpu.VMEM((samples - rows, targets), jnp.float32),
                pltpu.VMEM((targets, samples - rows), jnp.float32),
                dma((CHUNKS,)), dma((CHUNKS,)), dma((CHUNKS,)), dma((2, V_SLOTS)),
                dma((2, half)), dma((2, half)), dma((2, CHUNKS)), dma((2, CHUNKS)), dma((2, half)), dma((2, half)),
                dma((SWEEPS, ns - 1)), dma((SWEEPS, ns - 1)),
                dma((SWEEPS + 1, nf - 1)), dma((SWEEPS + 1, nf - 1)),
                dma((SWEEPS, ns - 1)), dma((SWEEPS, ns - 1)),
                dma((2, CHUNKS)), dma((2, CHUNKS)), dma((2, half)), dma((2, half)),
            ],
            compiler_params=pltpu.CompilerParams(collective_id=0, has_side_effects=True, vmem_limit_bytes=47 * 1024 * 1024),
            cost_estimate=pl.CostEstimate(flops=2 * rows * small * (2 * SWEEPS + 1), bytes_accessed=8 * small + 4 * rows * feat_len,
                                          transcendentals=0),
            name="ridge_sweeps",
        )(x_loc, w_loc.T, y_loc.T, eta_loc.reshape(1, feat_len))
        pieces = 8

        def put(w_ref, r_ref, w_hbm, r_hbm, sem):
            width = feat_len // pieces
            copies = [pltpu.make_async_copy(w_ref.at[:, pl.ds(i * width, width)], w_hbm.at[:, pl.ds(i * width, width)], sem.at[i])
                      for i in range(pieces)]
            copies.append(pltpu.make_async_copy(r_ref, r_hbm, sem.at[pieces]))
            for copy in copies:
                copy.start()
            for copy in copies:
                copy.wait()

        w_out, r_out = pl.pallas_call(
            put,
            out_shape=(jax.ShapeDtypeStruct((targets, feat_len), jnp.float32), jax.ShapeDtypeStruct((targets, rows), jnp.float32)),
            in_specs=[vmem, vmem],
            out_specs=(hbm, hbm),
            scratch_shapes=[dma((pieces + 1,))],
            compiler_params=pltpu.CompilerParams(vmem_limit_bytes=1024 * 1024),
            name="put_results",
        )(pltpu.with_memory_space_constraint(w_out, pltpu.VMEM), pltpu.with_memory_space_constraint(r_out, pltpu.VMEM))
        return w_out.T, r_out.T

    return jax.shard_map(
        local_solve,
        mesh=mesh,
        in_specs=(P(("prob", "samp"), "feat"), P(("prob", "feat"), None), P(("prob", "samp"), None), P(("prob", "feat"))),
        out_specs=(P(("prob", "feat"), None), P(("prob", "samp"), None)),
        check_vma=False,
    )
```

```python
import functools

import jax
import jax.numpy as jnp
from jax import lax
from jax.experimental import pallas as pl
from jax.experimental.pallas import tpu as pltpu
from jax.sharding import PartitionSpec as P

SWEEPS = 4
COMBINE_WEIGHT = 0.8
RIDGE_SCALE = 0.1
CHUNKS = 16
SUB = 512
STREAM = 0.5
V_SLOTS = 3
MESH = pl.DeviceIdType.MESH
NT = (((1,), (1,)), ((), ()))


BLOCK = (0, 2, 1, 3)


def far_first(count):
    return sorted(range(1, count), key=lambda o: -min(o, count - o))


def kernel(ns, nf, x_hbm, wt_hbm, yt_ref, eta_hbm, wout, rout, relay, xbuf, gbuf, dbuf, ebuf, vx, vw, usend, rsbuf, agbuf, rbuf, rstate, ucol, urow,
           own_sem, w_sem, e_sem, v_sem, rel_s, rel_r, dir_s, dir_r, fwd_s, fwd_r, a_s, a_r, b_s, b_r, c_s, c_r,
           wd_s, wd_r, wf_s, wf_r):
    y, f = lax.axis_index("samp"), lax.axis_index("feat")
    rows, feat_len = x_hbm.shape
    targets = wt_hbm.shape[0]
    own = feat_len // ns
    chunk = own // CHUNKS
    half, quarter = CHUNKS // 2, CHUNKS // 4
    sub = min(SUB, chunk)
    samples = rows * ns
    inv = 1.0 / samples
    ridge = RIDGE_SCALE * (feat_len * nf) / samples
    up, down, far = lax.rem(y + 1, ns), lax.rem(y + ns - 1, ns), lax.rem(y + 2, ns)
    ring = (up, down)

    def cols(owner, k):
        return pl.ds(pl.multiple_of(owner * own + k * chunk, chunk), chunk)

    def block_cols(owner, i):
        return pl.ds(pl.multiple_of(owner * own + i * 2 * chunk, 2 * chunk), 2 * chunk)

    def lanes(h, part):
        return pl.ds(h * chunk + part.start, part.size)

    def rows_of(o):
        return pl.ds(BLOCK[o] * rows, rows)

    def remote(src, dst, send, recv, axis, dev):
        return pltpu.make_async_remote_copy(src_ref=src, dst_ref=dst, send_sem=send, recv_sem=recv,
                                            device_id={axis: dev}, device_id_type=MESH)

    def own_copy(i):
        return pltpu.make_async_copy(x_hbm.at[:, block_cols(y, i)], xbuf.at[i, rows_of(0), :], own_sem.at[i])

    def w_load(k):
        return pltpu.make_async_copy(wt_hbm.at[:, cols(y, k)], wout.at[:, cols(y, k)], w_sem.at[k])

    def e_load(k):
        return pltpu.make_async_copy(eta_hbm.at[:, cols(y, k)], ebuf.at[k], e_sem.at[k])

    v_steps = ns * CHUNKS

    def v_cols(k):
        return pl.ds(pl.multiple_of(k * chunk, chunk), chunk)

    def v_load(k, slot):
        return (pltpu.make_async_copy(x_hbm.at[:, v_cols(k)], vx.at[slot], v_sem.at[0, slot]),
                pltpu.make_async_copy(wt_hbm.at[:, v_cols(k)], vw.at[slot], v_sem.at[1, slot]))

    def relay_copy(d, p):
        return remote(x_hbm.at[:, block_cols(far, 2 * p + d)], relay.at[d, p], rel_s.at[d, p], rel_r.at[d, p], "samp", ring[d])

    def direct_copy(d, i):
        return remote(x_hbm.at[:, block_cols(ring[d], i)], xbuf.at[i, rows_of((ns - 1, 1)[d]), :], dir_s.at[d, i], dir_r.at[d, i],
                      "samp", ring[d])

    def forward_copy(d, p, h):
        return remote(relay.at[d, p, :, pl.ds(h * chunk, chunk)], xbuf.at[2 * p + d, rows_of(2), pl.ds(h * chunk, chunk)],
                      fwd_s.at[d, 2 * p + h], fwd_r.at[d, 2 * p + h], "samp", ring[d])

    def wd_copy(d, k, owner):
        return remote(wout.at[:, cols(y, k)], wout.at[:, cols(owner, k)], wd_s.at[d, k], wd_r.at[d, k], "samp", ring[d])

    def wf_copy(d, i, owner):
        part = wout.at[:, cols(owner, 2 * i + d)]
        return remote(part, part, wf_s.at[d, i], wf_r.at[d, i], "samp", ring[d])

    def each(count, body):
        lax.fori_loop(0, count, lambda i, c: (body(i), c)[1], 0)

    def start_local(k):
        w_load(k).start()
        e_load(k).start()

    barrier = pltpu.get_barrier_semaphore()
    for o in range(1, ns):
        pl.semaphore_signal(barrier, inc=1, device_id={"samp": lax.rem(y + o, ns)}, device_id_type=MESH)
    for o in range(1, nf):
        pl.semaphore_signal(barrier, inc=1, device_id={"feat": lax.rem(f + o, nf)}, device_id_type=MESH)
    for k in range(V_SLOTS):
        for copy in v_load(k, k):
            copy.start()
    pl.semaphore_wait(barrier, ns - 1 + nf - 1)

    def start_relay(i):
        for d in range(2):
            relay_copy(d, i).start()

    each(quarter, start_relay)

    def v_step(k, acc):
        slot = lax.rem(k, V_SLOTS)
        for copy in v_load(k, slot):
            copy.wait()
        low = vw[slot].astype(jnp.bfloat16)
        acc = acc + lax.dot_general(low, vx[slot], NT, preferred_element_type=jnp.float32)

        @pl.when(k + V_SLOTS < v_steps)
        def _():
            for copy in v_load(k + V_SLOTS, slot):
                copy.start()

        return acc

    first = lax.fori_loop(0, v_steps, v_step, jnp.zeros((targets, rows), jnp.float32))
    each(half, lambda i: own_copy(i).start())
    each(CHUNKS, start_local)

    def a_copy(t, o):
        return remote(usend.at[t, o], rsbuf.at[t, ns - o], a_s.at[t, o - 1], a_r.at[t, o - 1], "samp", lax.rem(y + o, ns))

    def b_copy(t, o, place):
        return remote(agbuf.at[t, f], agbuf.at[t, place], b_s.at[t, o - 1], b_r.at[t, o - 1], "feat", lax.rem(f + o, nf))

    def c_copy(t, o):
        return remote(rbuf.at[t, 0], rbuf.at[t, BLOCK[ns - o]], c_s.at[t, o - 1], c_r.at[t, o - 1], "samp", lax.rem(y + o, ns))

    def start_a(t, o):
        place = pl.ds((BLOCK[o] - 1) * rows, rows)
        usend[t, o] = ucol[place, :].T + urow[:, place]
        a_copy(t, o).start()

    def finish_a(t, total):
        for o in range(1, ns):
            a_copy(t, o).wait_recv()
        for o in range(1, ns):
            total = total + rsbuf[t, o]
        return total

    def sum_blocks(t, term):
        agbuf[t, f] = term.astype(jnp.bfloat16)
        for o in far_first(nf):
            b_copy(t, o, f).start()
        for o in range(1, nf):
            b_copy(t, o, lax.rem(f + nf - o, nf)).wait_recv()
        total = agbuf[t, 0].astype(jnp.float32)
        for j in range(1, nf):
            total = total + agbuf[t, j].astype(jnp.float32)
        return total

    def start_c(t):
        rbuf[t, 0] = rstate[...].astype(jnp.bfloat16)
        for o in far_first(ns):
            c_copy(t, o).start()

    def finish_c(t, offsets):
        for o in offsets:
            c_copy(t, o).wait_recv()
        return jnp.concatenate([rbuf[t, b] for b in sorted(BLOCK[o] for o in offsets)], axis=1)

    rstate[...] = yt_ref[...] - sum_blocks(0, first)
    start_c(0)

    def start_direct(k):
        for d in range(2):
            direct_copy(d, k).start()

    each(half, start_direct)

    def start_forward(p):
        for d in range(2):
            relay_copy(d, p).wait_recv()
        for h in range(2):
            for d in range(2):
                forward_copy(d, p, h).start()

    each(quarter, start_forward)

    parts = chunk // sub

    def rows_grad(low, first_row, i, h, part):
        held = pl.ds(first_row, low.shape[1])
        return jnp.dot(low, xbuf[i, held, lanes(h, part)], preferred_element_type=jnp.float32)

    def own_grad(low, i):
        for h in range(2):
            for s in range(parts):
                part = pl.ds(s * sub, sub)
                gbuf[2 * i + h, :, part] = rows_grad(low, 0, i, h, part)

    def ready_grad(own_low, near_low, i):
        own_copy(i).wait()
        for e in range(2):
            direct_copy(e, i).wait_recv()
        for h in range(2):
            for s in range(parts):
                part = pl.ds(s * sub, sub)
                gbuf[2 * i + h, :, part] = rows_grad(own_low, 0, i, h, part) + rows_grad(near_low, 2 * rows, i, h, part)

    def advance(i, h, s, low):
        k = 2 * i + h
        part = pl.ds(s * sub, sub)
        grad = (gbuf[k, :, part] + rows_grad(low, rows, i, h, part)) * inv
        place = pl.ds(pl.multiple_of(y * own + k * chunk + s * sub, sub), sub)
        w_part = wout[:, place]
        delta = ebuf[k, :, part] * (grad - ridge * w_part)
        wout[:, place] = w_part + COMBINE_WEIGHT * delta
        low = delta.astype(jnp.bfloat16)
        dbuf[k, :, part] = low
        return low

    def other_rows(first_row, i, h, low_of):
        col, row = None, None
        for s in range(parts):
            low = low_of(s)
            x_part = xbuf[i, first_row:, lanes(h, pl.ds(s * sub, sub))]
            if s < STREAM * parts:
                term = lax.dot_general(x_part, low, NT, preferred_element_type=jnp.float32)
                col = term if col is None else col + term
            else:
                term = lax.dot_general(low, x_part, NT, preferred_element_type=jnp.float32)
                row = term if row is None else row + term
        if col is not None:
            ucol[first_row - rows:, :] += col
        if row is not None:
            urow[:, first_row - rows:] += row


    def own_rows(i, acc):
        for h in range(2):
            for s in range(0, parts, 1):
                part = pl.ds(s * sub, 1 * sub)
                acc = acc + lax.dot_general(xbuf[i, :rows, lanes(h, part)], dbuf[2 * i + h, :, part], NT, preferred_element_type=jnp.float32)
        return acc

    def near_rows(i, carry):
        col, row = carry
        for h in range(2):
            k, held = 2 * i + h, pl.ds(h * chunk, chunk)
            col = col + lax.dot_general(xbuf[i, 2 * rows:3 * rows, held], dbuf[k], NT, preferred_element_type=jnp.float32)
            row = row + lax.dot_general(dbuf[k], xbuf[i, 3 * rows:, held], NT, preferred_element_type=jnp.float32)
        return col, row

    def pair_rows(first_row, last_row, i):
        col, row = None, None
        held, out = pl.ds(first_row, last_row - first_row), pl.ds(first_row - rows, last_row - first_row)
        for s in range(0, parts, 1):
            part = pl.ds(s * sub, 1 * sub)
            term = lax.dot_general(xbuf[i, held, lanes(0, part)], dbuf[2 * i, :, part], NT, preferred_element_type=jnp.float32)
            col = term if col is None else col + term
            term = lax.dot_general(dbuf[2 * i + 1, :, part], xbuf[i, held, lanes(1, part)], NT, preferred_element_type=jnp.float32)
            row = term if row is None else row + term
        ucol[out, :] += col
        urow[:, out] += row

    def arriving(low, p):
        for h in range(2):
            for d in range(2):
                i = 2 * p + d
                w_load(2 * i + h).wait()
                e_load(2 * i + h).wait()
                forward_copy(d, p, h).wait_recv()
                other_rows(rows, i, h, lambda s: advance(i, h, s, low))

    def staying(low, i):
        for h in range(2):
            for s in range(parts):
                advance(i, h, s, low)

    def send_w(k):
        for d in range(2):
            wd_copy(d, k, y).start()

    def leaving(low, i):
        for s in range(parts):
            advance(i, 0, s, low)

        @pl.when(i > 0)
        def _():
            send_w(2 * i - 1)

        for s in range(parts):
            advance(i, 1, s, low)
        send_w(2 * i)

    for t in range(SWEEPS):
        ucol[...] = jnp.zeros_like(ucol)
        urow[...] = jnp.zeros_like(urow)
        if t == 0:
            near = finish_c(t, (1, ns - 1))
            each(half, functools.partial(ready_grad, rbuf[t, 0], near))
            each(quarter, functools.partial(arriving, finish_c(t, (2,))))
            start_a(t, 2)
        else:
            each(half, functools.partial(own_grad, rbuf[t, 0]))
            other_low = finish_c(t, (1, 2, ns - 1))
            if t < SWEEPS - 1:
                each(half, functools.partial(staying, other_low))
            else:
                each(half, functools.partial(leaving, other_low))
                send_w(CHUNKS - 1)
            each(half, functools.partial(pair_rows, rows, 2 * rows))
            start_a(t, 2)
            zeros = jnp.zeros((rows, targets), jnp.float32), jnp.zeros((targets, rows), jnp.float32)
            ucol[rows:2 * rows, :], urow[:, 2 * rows:] = lax.fori_loop(0, half, near_rows, zeros)
        start_a(t, 1)
        start_a(t, ns - 1)
        mine = lax.fori_loop(0, half, own_rows, jnp.zeros((rows, targets), jnp.float32)).T
        if t < SWEEPS - 1:
            rstate[...] = rstate[...] - COMBINE_WEIGHT * sum_blocks(t + 1, finish_a(t, mine))
            start_c(t + 1)

    def start_wf(i):
        for d in range(2):
            k = 2 * i + d
            for e in range(2):
                wd_copy(e, k, ring[1 - e]).wait_recv()
            wf_copy(d, i, ring[1 - d]).start()

    def start_wf_pair(i):
        start_wf(i)

    each(half, start_wf_pair)
    rout[...] = rstate[...] - COMBINE_WEIGHT * sum_blocks(SWEEPS, finish_a(SWEEPS - 1, mine))

    def finish_full(k):
        for d in range(2):
            wd_copy(d, k, y).wait_send()

    def finish_half(i):
        for d in range(2):
            direct_copy(d, i).wait_send()

    def finish_quarter(p):
        for d in range(2):
            relay_copy(d, p).wait_send()
            for h in range(2):
                forward_copy(d, p, h).wait_send()

    def finish_last(i):
        for d in range(2):
            wf_copy(d, i, ring[1 - d]).wait_send()
            wf_copy(d, i, far).wait_recv()

    each(CHUNKS, finish_full)
    each(half, finish_half)
    each(quarter, finish_quarter)
    for t in range(SWEEPS):
        for o in range(1, ns):
            a_copy(t, o).wait_send()
            c_copy(t, o).wait_send()
    for t in range(SWEEPS + 1):
        for o in range(1, nf):
            b_copy(t, o, f).wait_send()
    each(half, finish_last)


def solution(mesh):
    ns, nf = mesh.shape["samp"], mesh.shape["feat"]

    def local_solve(x_loc, w_loc, y_loc, eta_loc):
        rows, feat_len = x_loc.shape
        targets = w_loc.shape[1]
        samples = rows * ns
        chunk = feat_len // ns // CHUNKS
        half, quarter = CHUNKS // 2, CHUNKS // 4
        dma = pltpu.SemaphoreType.DMA
        hbm = pl.BlockSpec(memory_space=pl.ANY)
        vmem = pl.BlockSpec(memory_space=pltpu.VMEM)
        small = feat_len * targets
        w_out, r_out, _ = pl.pallas_call(
            functools.partial(kernel, ns, nf),
            out_shape=(pltpu.VMEM((targets, feat_len), jnp.float32), pltpu.VMEM((targets, rows), jnp.float32),
                       jax.ShapeDtypeStruct((2, quarter, rows, 2 * chunk), jnp.bfloat16)),
            in_specs=[hbm, hbm, vmem, hbm],
            out_specs=(vmem, vmem, hbm),
            scratch_shapes=[
                pltpu.VMEM((half, samples, 2 * chunk), jnp.bfloat16),
                pltpu.VMEM((CHUNKS, targets, chunk), jnp.float32),
                pltpu.VMEM((CHUNKS, targets, chunk), jnp.bfloat16),
                pltpu.VMEM((CHUNKS, 1, chunk), jnp.float32),
                pltpu.VMEM((V_SLOTS, rows, chunk), jnp.bfloat16),
                pltpu.VMEM((V_SLOTS, targets, chunk), jnp.float32),
                pltpu.VMEM((SWEEPS, ns, targets, rows), jnp.float32),
                pltpu.VMEM((SWEEPS, ns, targets, rows), jnp.float32),
                pltpu.VMEM((SWEEPS + 1, nf, targets, rows), jnp.bfloat16),
                pltpu.VMEM((SWEEPS, ns, targets, rows), jnp.bfloat16),
                pltpu.VMEM((targets, rows), jnp.float32),
                pltpu.VMEM((samples - rows, targets), jnp.float32),
                pltpu.VMEM((targets, samples - rows), jnp.float32),
                dma((half,)), dma((CHUNKS,)), dma((CHUNKS,)), dma((2, V_SLOTS)),
                dma((2, quarter)), dma((2, quarter)), dma((2, half)), dma((2, half)), dma((2, half)), dma((2, half)),
                dma((SWEEPS, ns - 1)), dma((SWEEPS, ns - 1)),
                dma((SWEEPS + 1, nf - 1)), dma((SWEEPS + 1, nf - 1)),
                dma((SWEEPS, ns - 1)), dma((SWEEPS, ns - 1)),
                dma((2, CHUNKS)), dma((2, CHUNKS)), dma((2, half)), dma((2, half)),
            ],
            compiler_params=pltpu.CompilerParams(collective_id=0, has_side_effects=True, vmem_limit_bytes=47 * 1024 * 1024),
            cost_estimate=pl.CostEstimate(flops=2 * rows * small * (2 * SWEEPS + 1), bytes_accessed=8 * small + 4 * rows * feat_len,
                                          transcendentals=0),
            name="ridge_sweeps",
        )(x_loc, w_loc.T, y_loc.T, eta_loc.reshape(1, feat_len))
        pieces = 8

        def put(w_ref, r_ref, w_hbm, r_hbm, sem):
            width = feat_len // pieces
            copies = [pltpu.make_async_copy(w_ref.at[:, pl.ds(i * width, width)], w_hbm.at[:, pl.ds(i * width, width)], sem.at[i])
                      for i in range(pieces)]
            copies.append(pltpu.make_async_copy(r_ref, r_hbm, sem.at[pieces]))
            for copy in copies:
                copy.start()
            for copy in copies:
                copy.wait()

        w_out, r_out = pl.pallas_call(
            put,
            out_shape=(jax.ShapeDtypeStruct((targets, feat_len), jnp.float32), jax.ShapeDtypeStruct((targets, rows), jnp.float32)),
            in_specs=[vmem, vmem],
            out_specs=(hbm, hbm),
            scratch_shapes=[dma((pieces + 1,))],
            compiler_params=pltpu.CompilerParams(vmem_limit_bytes=1024 * 1024),
            name="put_results",
        )(pltpu.with_memory_space_constraint(w_out, pltpu.VMEM), pltpu.with_memory_space_constraint(r_out, pltpu.VMEM))
        return w_out.T, r_out.T

    return jax.shard_map(
        local_solve,
        mesh=mesh,
        in_specs=(P(("prob", "samp"), "feat"), P(("prob", "feat"), None), P(("prob", "samp"), None), P(("prob", "feat"))),
        out_specs=(P(("prob", "feat"), None), P(("prob", "samp"), None)),
        check_vma=False,
    )
```
